256 devices in a mesh: band: 16 (over y_lo, z), grid: 16 (over x, y_hi, core).
Axes of the slice: x: 4, y: 4 (y_hi: 2, y_lo: 2; y = y_hi * 2 + y_lo), z: 8, core: 2. Of those that a mesh axis runs over, the one named last changes fastest.
Arguments:
- bands: bfloat16 [2, 32, 128, 128, 128], P(None, 'band', 'grid'), may hold values from -6 to 6
- occupations: float32 [32], P('band'), may hold values from 0.25 to 1
- external: float32 [128, 128, 128], P('grid'), may hold values from 0 to 2
- density_in: float32 [128, 128, 128], P('grid'), may hold values from -0.2 to 1.4
- prev_density: float32 [128, 128, 128], P('grid'), may hold values from 0 to 1.2
- prev_residual: float32 [128, 128, 128], P('grid'), may hold values from -1.3 to 0.3
- hist_density: float32 [5, 128, 128, 128], P(None, 'grid'), may hold values from 0 to 1
- hist_residual: float32 [5, 128, 128, 128], P(None, 'grid'), may hold values from -0.6 to 1
Outputs:
- density: float32 [128, 128, 128], P('grid')
- residual: float32 [128, 128, 128], P('grid')
The draws below stay inside these ranges and needn't reach their ends.
All inputs are finite; a program needn't handle non-finite values.
Results may differ from the reference program's by a relative error of at most 0.018.
The reference program's roundings to bfloat16 on the way count: a program that leaves them out, or rounds other values in their place, can miss the bound.
Values may be sent and summed in bfloat16 or wider, within the bound.
A program may use at most 128 MiB of HBM per device.

```python
import math
import jax
import jax.numpy as jnp
from jax import lax

NG = 128
DEPTH = 6
ITERS = 3
BANDS = 32


def draw_density_in(key, part):
    jitter = jax.random.uniform(key, (NG, NG, NG), jnp.float32, -0.4, 0.4)
    position = jnp.arange(NG, dtype=jnp.float32)[:, None, None] / (NG - 1)
    return 0.2 + 0.8 * position + jitter


def draw_prev_residual(key, part):
    jitter = jax.random.uniform(jax.random.fold_in(key, 11), (NG, NG, NG), jnp.float32, -0.3, 0.3)
    position = jnp.arange(NG, dtype=jnp.float32)[:, None, None] / (NG - 1)
    return -(0.2 + 0.8 * position) + jitter


def draw_hist_residual(key, part):
    jitter = jax.random.uniform(jax.random.fold_in(key, 23), (DEPTH - 1, NG, NG, NG), jnp.float32, -0.3, 0.3)
    position = jnp.arange(NG, dtype=jnp.float32) / (NG - 1)
    order = DEPTH - 1 - jnp.arange(DEPTH - 1, dtype=jnp.float32)
    profile = 0.2 + 0.5 * jnp.cos(math.pi * order[:, None] * position[None, :])
    return profile[:, :, None, None] + jitter


def level_of(rng, shape, cuts, least, largest):
    level = 1.0
    for axis_at, parts in cuts:
        draws = jax.random.uniform(jax.random.fold_in(jax.random.fold_in(rng, 6), axis_at), (parts,), jnp.float32, least / len(cuts), largest / len(cuts))
        level = level * jnp.repeat(jnp.exp(draws), shape[axis_at] // parts).reshape((-1,) + (1,) * (len(shape) - 1 - axis_at))
    return level


def scatter_about(key, shape, spread, reach, shards=(), held_as=jnp.bfloat16):
    entries = jax.random.normal(key, shape, jnp.float32) * spread
    if len(shards) > 0:
        entries = level_of(key, shape, shards, -0.22, 0.18) * entries
    return jnp.clip(entries, min=-reach, max=reach).astype(held_as)


def setup_inputs(seed: int = 0) -> dict:
    streams_of = jax.random.split(jax.random.key(seed), 9)
    bands = scatter_about(streams_of[0], (2, BANDS, NG, NG, NG), 1.0, 6.0, ((1, 16), (2, 16)))
    occupations = jnp.clip(jnp.exp(math.log(1.0) - 1.3862944 * jax.random.uniform(streams_of[1], (BANDS,), jnp.float32) ** level_of(streams_of[1], (BANDS,), ((0, 16),), -0.2, 0.2)), 0.25, 1.0)
    external = jnp.clip(2.0 * jax.random.uniform(streams_of[2], (NG, NG, NG), jnp.float32) ** level_of(streams_of[2], (NG, NG, NG), ((0, 16),), -0.2, 0.2), 0.0, 2.0)
    density_in = draw_density_in(jax.random.fold_in(streams_of[8], 71), 0)
    prev_density = jnp.clip(1.2 * jax.random.uniform(streams_of[4], (NG, NG, NG), jnp.float32) ** level_of(streams_of[4], (NG, NG, NG), ((0, 16),), -0.2, 0.2), 0.0, 1.2)
    prev_residual = draw_prev_residual(jax.random.fold_in(streams_of[8], 71), 0)
    hist_density = jnp.clip(1.0 * jax.random.uniform(streams_of[6], (DEPTH - 1, NG, NG, NG), jnp.float32) ** level_of(streams_of[6], (DEPTH - 1, NG, NG, NG), ((1, 16),), -0.2, 0.2), 0.0, 1.0)
    hist_residual = draw_hist_residual(jax.random.fold_in(streams_of[8], 71), 0)
    return dict(bands=bands, occupations=occupations, external=external, density_in=density_in, prev_density=prev_density, prev_residual=prev_residual, hist_density=hist_density, hist_residual=hist_residual)


time_step = 0.25
energy_shift = 2.5
coupling = 1.0
mixing_weight = 0.5
ridge_share = 0.1
ridge_floor = 0.01
density_scale = 8.0
highest = lax.Precision.HIGHEST

def fourier_tables(length, frequency):
    positions = jnp.arange(length, dtype=jnp.int32)
    phase_index = positions[:, None] * frequency[None, :] % length
    angles = phase_index.astype(jnp.float32) * (2.0 * math.pi / length)
    unit_scale = 1.0 / math.sqrt(length)
    return ((jnp.cos(angles) * unit_scale).astype(jnp.bfloat16), (jnp.sin(angles) * unit_scale).astype(jnp.bfloat16))

def solve_definite(matrix, vector):
    extent = matrix.shape[0]
    factor_low = jnp.zeros_like(matrix)
    for column in range(extent):
        pivot_value = jnp.sqrt(matrix[column, column] - jnp.sum(factor_low[column, :column] * factor_low[column, :column]))
        factor_low = factor_low.at[column, column].set(pivot_value)
        for row_index in range(column + 1, extent):
            element = (matrix[row_index, column] - jnp.sum(factor_low[row_index, :column] * factor_low[column, :column])) / pivot_value
            factor_low = factor_low.at[row_index, column].set(element)
    middle = jnp.zeros_like(vector)
    for row_index in range(extent):
        element = (vector[row_index] - jnp.sum(factor_low[row_index, :row_index] * middle[:row_index])) / factor_low[row_index, row_index]
        middle = middle.at[row_index].set(element)
    result = jnp.zeros_like(vector)
    for row_index in reversed(range(extent)):
        element = (middle[row_index] - jnp.sum(factor_low[row_index + 1:, row_index] * result[row_index + 1:])) / factor_low[row_index, row_index]
        result = result.at[row_index].set(element)
    return result

def contract(operand, matrix):
    return jnp.einsum('abl,lk->abk', operand, matrix, precision=highest)

def along_axis(real_part, imag_part, cosine_part, sine_part, orientation, axis_index):
    cosine_wide = cosine_part.astype(jnp.float32)
    sine_wide = sine_part.astype(jnp.float32) * orientation
    real_moved = jnp.moveaxis(real_part.astype(jnp.float32), axis_index, -1)
    imag_moved = jnp.moveaxis(imag_part.astype(jnp.float32), axis_index, -1)
    out_real = contract(real_moved, cosine_wide) - contract(imag_moved, sine_wide)
    out_imag = contract(real_moved, sine_wide) + contract(imag_moved, cosine_wide)
    return (jnp.moveaxis(out_real, -1, axis_index), jnp.moveaxis(out_imag, -1, axis_index))

def band_step(real_part, imag_part, factor, kinetic, tables):
    cosine_part, sine_part = tables
    real_part = (real_part.astype(jnp.float32) * factor).astype(jnp.bfloat16)
    imag_part = (imag_part.astype(jnp.float32) * factor).astype(jnp.bfloat16)
    for axis_index in (2, 1):
        real_part, imag_part = along_axis(real_part, imag_part, cosine_part, sine_part, -1.0, axis_index)
        real_part = real_part.astype(jnp.bfloat16)
        imag_part = imag_part.astype(jnp.bfloat16)
    real_part, imag_part = along_axis(real_part, imag_part, cosine_part, sine_part, -1.0, 0)
    real_part = (real_part * kinetic).astype(jnp.bfloat16)
    imag_part = (imag_part * kinetic).astype(jnp.bfloat16)
    for axis_index in (0, 1, 2):
        real_part, imag_part = along_axis(real_part, imag_part, cosine_part.T, sine_part.T, 1.0, axis_index)
        real_part = real_part.astype(jnp.bfloat16)
        imag_part = imag_part.astype(jnp.bfloat16)
    return (real_part, imag_part)

def reference(bands, occupations, external, density_in, prev_density, prev_residual, hist_density, hist_residual):
    frequency = jnp.arange(-(NG // 4), NG // 4, dtype=jnp.int32)
    tables = fourier_tables(NG, frequency)
    squared = frequency.astype(jnp.float32) * frequency.astype(jnp.float32)
    quarter = NG / 4.0
    radius = squared[:, None, None] + squared[None, :, None] + squared[None, None, :]
    kinetic = jnp.exp(-time_step * radius / (quarter * quarter))
    cells_total = NG * NG * NG
    real_bands = bands[0]
    imag_bands = bands[1]
    density_now = density_in
    density_prev = prev_density
    residual_prev = prev_residual
    density_diffs = hist_density
    residual_diffs = hist_residual
    residual = density_in
    for iteration in range(ITERS):
        factor = jnp.exp(-time_step * (external + coupling * density_now - energy_shift))

        def one_band(accumulated, slices):
            real_part, imag_part, weight = slices
            real_part, imag_part = band_step(real_part, imag_part, factor, kinetic, tables)
            wide_real = real_part.astype(jnp.float32)
            wide_imag = imag_part.astype(jnp.float32)
            return (accumulated + weight * (wide_real * wide_real + wide_imag * wide_imag), (real_part, imag_part))
        accumulated, (real_bands, imag_bands) = lax.scan(one_band, jnp.zeros((NG, NG, NG), jnp.float32), (real_bands, imag_bands, occupations))
        density_out = accumulated * (density_scale / BANDS)
        residual = density_out - density_now
        density_diffs = jnp.concatenate([density_diffs[density_diffs.shape[0] - (DEPTH - 1):], (density_now - density_prev)[None]], axis=0)
        residual_diffs = jnp.concatenate([residual_diffs[residual_diffs.shape[0] - (DEPTH - 1):], (residual - residual_prev)[None]], axis=0)
        flat_diffs = residual_diffs.reshape(DEPTH, -1)
        gram_matrix = jnp.dot(flat_diffs, flat_diffs.T, precision=highest) / cells_total
        right_side = jnp.dot(flat_diffs, residual.reshape(-1), precision=highest) / cells_total
        ridge_value = ridge_share * jnp.trace(gram_matrix) / DEPTH + ridge_floor
        coeffs = solve_definite(gram_matrix + ridge_value * jnp.eye(DEPTH, dtype=jnp.float32), right_side)
        combined = density_diffs + mixing_weight * residual_diffs
        density_next = density_now + mixing_weight * residual - jnp.einsum('j,jxyz->xyz', coeffs, combined, precision=highest)
        density_prev = density_now
        residual_prev = residual
        density_now = density_next
    return (density_now, residual)
```

```python
import math

import jax
import jax.numpy as jnp
import ml_dtypes
import numpy as np
from jax import lax
from jax.experimental import pallas as pl
from jax.experimental.pallas import tpu as pltpu
from jax.sharding import PartitionSpec as P

NG = 128
KEPT = NG // 2
DEPTH = 6
ITERS = 3
F32 = jnp.float32
BF16 = jnp.bfloat16
MESH = pl.DeviceIdType.MESH

time_step = 0.25
energy_shift = 2.5
mixing_weight = 0.5
ridge_share = 0.1
ridge_floor = 0.01
density_scale = 8.0
bands_total = 32


def tables():
    frequency = np.arange(-(NG // 4), NG // 4, dtype=np.int32)
    positions = np.arange(NG, dtype=np.int32)
    phase = (positions[:, None] * frequency[None, :]) % NG
    angles = phase.astype(np.float32) * np.float32(2.0 * math.pi / NG)
    unit = np.float32(1.0 / math.sqrt(NG))
    cosine = (np.cos(angles) * unit).astype(ml_dtypes.bfloat16)
    sine = (np.sin(angles) * unit).astype(ml_dtypes.bfloat16)
    forward_z = np.concatenate(
        [np.concatenate([cosine, -sine], 1), np.concatenate([sine, cosine], 1)], 0
    )
    inverse_z = np.concatenate(
        [np.concatenate([cosine.T, sine.T], 1), np.concatenate([-sine.T, cosine.T], 1)], 0
    )
    stacked = np.concatenate([cosine.T, sine.T], 0)
    beside = np.concatenate([cosine, sine], 1)
    return forward_z, inverse_z, stacked, beside


def dot(a, b):
    return jnp.dot(a, b, preferred_element_type=F32)


def kernel(
    occ, bands, ext, den, pden, pres, hden, hres, wzf, wzi, fcs, ics,
    out_d, out_r,
    bands_v, ext_v, den_v, facg, facp, plane, rs, qs, psi,
    send_f, recv_f, stage, kin, send_b, recv_b, part, recv_d, row_s, rows, occ_s, occs,
    outs_s, outs_v,
    in_sems, pl_sems, pl_send, sf_sem, rf_sem, sb_sem, rb_sems, sd_sem, rd_sems,
    sr_sem, rr_sem, so_sem, ro_sem, sout_sems, rout_sems,
):
    g = lax.axis_index("band")
    i = lax.axis_index("grid")
    core = i % 2
    xy = i // 2
    half = g // 8
    zz = g % 8
    me = xy * 16 + g
    twin = i + 1 - 2 * core

    def remote(src, dst, ssem, rsem, dg, di):
        return pltpu.make_async_remote_copy(
            src_ref=src, dst_ref=dst, send_sem=ssem, recv_sem=rsem,
            device_id=(dg, di), device_id_type=MESH,
        )

    def drain(ref, sem):
        pltpu.make_async_copy(ref, ref, sem).wait()

    loads = [
        pltpu.make_async_copy(ext, ext_v, in_sems.at[0]),
        pltpu.make_async_copy(den, den_v, in_sems.at[1]),
        pltpu.make_async_copy(bands, bands_v, in_sems.at[2]),
    ]
    for load in loads:
        load.start()

    owner = core == half

    @pl.when(owner)
    def _():
        pieces = [
            (ext.at[zz], plane.at[0], 0), (den.at[zz], plane.at[1], 0),
            (pden.at[zz], plane.at[2], 0), (pres.at[zz], plane.at[3], 0),
            (hden.at[:, zz], rs.at[pl.ds(0, DEPTH - 1)], 1),
            (hres.at[:, zz], qs.at[pl.ds(0, DEPTH - 1)], 2),
        ]
        for src, dst, s in pieces:
            pltpu.make_async_copy(src, dst, pl_sems.at[s]).start()
            remote(src, dst, pl_send.at[s], pl_sems.at[s], g, twin).start()

    occ_row = jnp.full((1, NG), occ[core], F32)
    occ_s[...] = occ_row
    occs[g] = occ_row

    def send_occ(n, c):
        remote(occ_s, occs.at[g], so_sem, ro_sem, (g + n) % 16, i).start()
        return c

    lax.fori_loop(1, 16, send_occ, 0)

    lane = lax.broadcasted_iota(jnp.int32, (KEPT, NG), 1)
    sgn_f = jnp.where(lane < KEPT, 1.0, -1.0).astype(F32)
    sgn_i = -sgn_f
    fz = (lane % KEPT - NG // 4).astype(F32)
    fx = (lax.broadcasted_iota(jnp.int32, (KEPT, NG), 0) - NG // 4).astype(F32)
    quarter = NG / 4.0
    for r in range(8):
        fy = (8 * xy + r - NG // 4).astype(F32)
        kin[r] = jnp.exp((fx * fx + fy * fy + fz * fz) * (-time_step / (quarter * quarter)))

    def forward_zy(w):
        a = dot(w, wzf[...]).astype(BF16)
        pq = dot(fcs[...], a)
        b = pq[:KEPT] + pltpu.roll(pq[KEPT:], KEPT, 1) * sgn_f
        return b.reshape(8, 8, NG).astype(BF16)

    def send_tile(src, dst, ssem, rsem, dg, di, same):
        @pl.when(same)
        def _():
            pltpu.make_async_copy(src, dst, rsem).start()

        @pl.when(jnp.logical_not(same))
        def _():
            remote(src, dst, ssem, rsem, dg, di).start()

    def spectral():
        drain(recv_f, rf_sem)
        stage[...] = recv_f[...].astype(F32).reshape(8 * NG, NG)
        for r in range(8):
            x = stage[pl.ds(r, NG, stride=8), :].astype(BF16)
            pq = dot(fcs[...], x)
            c = (pq[:KEPT] + pltpu.roll(pq[KEPT:], KEPT, 1) * sgn_f) * kin[r]
            c2 = pltpu.roll(c, KEPT, 1) * sgn_i
            both = jnp.concatenate([c, c2], axis=0).astype(BF16)
            stage[pl.ds(r, NG, stride=8), :] = dot(ics[...], both)
        send_b[...] = stage[...].reshape(NG, 8, NG).astype(BF16)

        def send(n, carry):
            p = (me + n) % 128
            send_tile(
                send_b.at[p], recv_b.at[g * 8 + xy], sb_sem, rb_sems.at[g],
                p % 16, 2 * (p // 16) + core, n == 0,
            )
            return carry

        lax.fori_loop(0, 128, send, 0)

    def backward(n, carry):
        t = (g + n) % 16
        tiles = recv_b.at[pl.ds(t * 8, 8)]
        drain(tiles, rb_sems.at[t])
        d = tiles[...].astype(F32).reshape(KEPT, NG)
        d2 = pltpu.roll(d, KEPT, 1) * sgn_i
        both = jnp.concatenate([d, d2], axis=0).astype(BF16)
        e = dot(ics[...], both).astype(BF16)
        new = dot(e, wzi[...]).astype(BF16)
        psi[t] = new
        wide = new.astype(F32)
        re, im = wide[:, :NG], wide[:, NG:]
        part[...] += occs[t] * (re * re + im * im)
        return carry

    gram = None
    for step in range(ITERS):
        if step == 0:
            for load in loads:
                load.wait()
            facg[...] = jnp.exp(-time_step * (ext_v[...] + den_v[...] - energy_shift))

            def forward(n, carry):
                which, j = n // 8, n % 8
                f = facg[j]
                w = jnp.concatenate(
                    [bands_v[0, which, j].astype(F32) * f, bands_v[1, which, j].astype(F32) * f],
                    axis=1,
                ).astype(BF16)
                send_f[pl.ds(n * 8, 8)] = forward_zy(w)
                for m in range(8):
                    q = (xy + m) % 8
                    di = 2 * q + which
                    send_tile(
                        send_f.at[n * 8 + q], recv_f.at[8 * i + j], sf_sem, rf_sem, g, di, di == i
                    )
                return carry

            lax.fori_loop(0, 16, forward, 0)
            drain(send_f.at[pl.ds(0, 120)], sf_sem)
        else:
            def forward(n, carry):
                t = (g + n) % 16
                f = facp[...]
                w = (psi[t].astype(F32) * jnp.concatenate([f, f], axis=1)).astype(BF16)
                send_f[pl.ds(t * 8, 8)] = forward_zy(w)
                for m in range(8):
                    q = (xy + m) % 8
                    send_tile(
                        send_f.at[t * 8 + q], recv_f.at[me], sf_sem, rf_sem,
                        t, 2 * q + core, jnp.logical_and(n == 0, m == 0),
                    )
                return carry

            lax.fori_loop(0, 16, forward, 0)
            drain(send_f.at[pl.ds(0, 127)], sf_sem)

        spectral()

        if step == 0:
            drain(plane, pl_sems.at[0])
            drain(rs.at[pl.ds(0, DEPTH - 1)], pl_sems.at[1])
            drain(qs.at[pl.ds(0, DEPTH - 1)], pl_sems.at[2])
            drain(occs.at[pl.ds(0, 15)], ro_sem)
            drain(occs.at[pl.ds(0, 15)], so_sem)

            @pl.when(owner)
            def _():
                drain(plane, pl_send.at[0])
                drain(rs.at[pl.ds(0, DEPTH - 1)], pl_send.at[1])
                drain(qs.at[pl.ds(0, DEPTH - 1)], pl_send.at[2])

        part[...] = jnp.zeros_like(part)
        lax.fori_loop(0, 16, backward, 0)
        drain(send_b.at[pl.ds(0, 127)], sb_sem)

        swap = remote(part, recv_d.at[step], sd_sem, rd_sems.at[step], g, twin)
        swap.start()
        swap.wait()
        rho_out = (part[...] + recv_d[step]) * (density_scale / bands_total)
        rho_in = plane[1]
        res = rho_out - rho_in
        newest = res - plane[3]
        rs[DEPTH - 1 + step] = rho_in - plane[2]
        qs[DEPTH - 1 + step] = newest

        def rows_of(a):
            return a.reshape(16, 8, NG)

        lanes = lax.broadcasted_iota(jnp.int32, (1, NG), 1)
        row = jnp.zeros((1, NG), F32)

        def put(row, at, a, b):
            total = jnp.sum(jnp.sum(rows_of(a * b), axis=0), axis=0, keepdims=True)
            return jnp.where(lanes == at, jnp.sum(total, axis=1, keepdims=True), row)

        for j in range(DEPTH):
            q = qs[step + j]
            row = put(row, j, q, newest)
            row = put(row, DEPTH + j, q, res)
        if step == 0:
            at = 2 * DEPTH
            for a in range(DEPTH - 1):
                for b in range(a + 1):
                    row = put(row, at, qs[a], qs[b])
                    at += 1
        row_s[...] = row
        rows[me] = row

        def send_row(n, carry):
            p = (me + n) % 128
            remote(row_s, rows.at[me], sr_sem, rr_sem, p % 16, 2 * (p // 16) + core).start()
            return carry

        lax.fori_loop(1, 128, send_row, 0)

        def gather(value, which):
            outs_s[which] = value.astype(BF16)

            def send(n, carry):
                dg = (g + n) % 16
                di = 2 * xy + half
                same = jnp.logical_and(n == 0, di == i)
                send_tile(
                    outs_s.at[which, pl.ds(pl.multiple_of(core * KEPT, KEPT), KEPT)],
                    outs_v.at[which, 2 * zz + core],
                    sout_sems.at[which], rout_sems.at[which], dg, di, same,
                )
                return carry

            lax.fori_loop(0, 16, send, 0)

        if step == ITERS - 1:
            gather(res, 1)

        drain(rows.at[pl.ds(0, 127)], rr_sem)
        drain(rows.at[pl.ds(0, 127)], sr_sem)
        sums = jnp.sum(rows[...], axis=0) * (1.0 / (NG * NG * NG))

        def splat(at):
            return jnp.broadcast_to(sums[:, at : at + 1], (8, NG))

        border = [splat(j) for j in range(DEPTH)]
        right = [splat(DEPTH + j) for j in range(DEPTH)]
        if step == 0:
            at = 2 * DEPTH
            gram = []
            for a in range(DEPTH - 1):
                gram.append([splat(at + b) for b in range(a + 1)])
                at += a + 1
        else:
            gram = [[gram[a][b] for b in range(1, a + 1)] for a in range(1, DEPTH)]
        gram.append(border)
        trace = gram[0][0]
        for j in range(1, DEPTH):
            trace = trace + gram[j][j]
        ridge = trace * (ridge_share / DEPTH) + ridge_floor
        low = [[None] * DEPTH for _ in range(DEPTH)]
        scaled = [[None] * DEPTH for _ in range(DEPTH)]
        inverse = [None] * DEPTH
        for c in range(DEPTH):
            value = gram[c][c] + ridge
            for k in range(c):
                value = value - scaled[c][k] * low[c][k]
            inverse[c] = 1.0 / value
            for r in range(c + 1, DEPTH):
                value = gram[r][c]
                for k in range(c):
                    value = value - scaled[r][k] * low[c][k]
                scaled[r][c] = value
                low[r][c] = value * inverse[c]
        middle = []
        for r in range(DEPTH):
            value = right[r]
            for k in range(r):
                value = value - low[r][k] * middle[k]
            middle.append(value)
        coeffs = [None] * DEPTH
        for r in reversed(range(DEPTH)):
            value = middle[r] * inverse[r]
            for k in range(r + 1, DEPTH):
                value = value - low[k][r] * coeffs[k]
            coeffs[r] = value
        mixed = rows_of(rho_in + mixing_weight * res)
        for j in range(DEPTH):
            mixed = mixed - coeffs[j][None] * rows_of(rs[step + j] + mixing_weight * qs[step + j])
        rho = mixed.reshape(NG, NG)
        if step < ITERS - 1:
            plane[2] = rho_in
            plane[3] = res
            plane[1] = rho
            facp[...] = jnp.exp(-time_step * (plane[0] + rho - energy_shift))
        else:
            gather(rho, 0)
            for which, out in ((1, out_r), (0, out_d)):
                drain(outs_v.at[which], rout_sems.at[which])
                out[...] = outs_v[which].astype(F32).reshape(8, NG, NG)

                @pl.when(owner)
                def _():
                    drain(outs_v.at[which, pl.ds(0, 15)], sout_sems.at[which])

                @pl.when(jnp.logical_not(owner))
                def _():
                    drain(outs_v.at[which], sout_sems.at[which])


def local(bands, occupations, external, density_in, prev_density, prev_residual, hist_density, hist_residual):
    constants = [jnp.asarray(t) for t in tables()]
    slab = external.shape
    hbm = pl.BlockSpec(memory_space=pl.ANY)
    vmem = pl.BlockSpec(memory_space=pltpu.VMEM)
    smem = pl.BlockSpec(memory_space=pltpu.SMEM)
    dma = pltpu.SemaphoreType.DMA
    out = jax.ShapeDtypeStruct(slab, F32)
    return pl.pallas_call(
        kernel,
        out_shape=(out, out),
        in_specs=[smem] + [hbm] * 7 + [vmem] * 4,
        out_specs=(vmem, vmem),
        scratch_shapes=[
            pltpu.VMEM(bands.shape, BF16),
            pltpu.VMEM(slab, F32),
            pltpu.VMEM(slab, F32),
            pltpu.VMEM(slab, F32),
            pltpu.VMEM((NG, NG), F32),
            pltpu.VMEM((4, NG, NG), F32),
            pltpu.VMEM((DEPTH - 1 + ITERS, NG, NG), F32),
            pltpu.VMEM((DEPTH - 1 + ITERS, NG, NG), F32),
            pltpu.VMEM((16, NG, 2 * NG), BF16),
            pltpu.VMEM((128, 8, NG), BF16),
            pltpu.VMEM((128, 8, NG), BF16),
            pltpu.VMEM((8 * NG, NG), F32),
            pltpu.VMEM((8, KEPT, NG), F32),
            pltpu.VMEM((128, 8, NG), BF16),
            pltpu.VMEM((128, 8, NG), BF16),
            pltpu.VMEM((NG, NG), F32),
            pltpu.VMEM((ITERS, NG, NG), F32),
            pltpu.VMEM((1, NG), F32),
            pltpu.VMEM((128, 1, NG), F32),
            pltpu.VMEM((1, NG), F32),
            pltpu.VMEM((16, 1, NG), F32),
            pltpu.VMEM((2, NG, NG), BF16),
            pltpu.VMEM((2, 16, KEPT, NG), BF16),
            dma((3,)), dma((3,)), dma((3,)),
            dma(()), dma(()), dma(()), dma((16,)), dma(()), dma((ITERS,)),
            dma(()), dma(()), dma(()), dma(()), dma((2,)), dma((2,)),
        ],
        compiler_params=pltpu.CompilerParams(
            has_side_effects=True, vmem_limit_bytes=48 * 1024 * 1024
        ),
        name="scf",
    )(
        occupations, bands, external, density_in, prev_density, prev_residual,
        hist_density, hist_residual, *constants,
    )


def solution(mesh):
    placed = (
        P(None, "band", "grid", None, None),
        P("band"),
        P("grid", None, None),
        P("grid", None, None),
        P("grid", None, None),
        P("grid", None, None),
        P(None, "grid", None, None),
        P(None, "grid", None, None),
    )
    return jax.shard_map(
        local,
        mesh=mesh,
        in_specs=placed,
        out_specs=(P("grid", None, None), P("grid", None, None)),
        check_vma=False,
    )
```

```python
import math

import jax
import jax.numpy as jnp
import ml_dtypes
import numpy as np
from jax import lax
from jax.experimental import pallas as pl
from jax.experimental.pallas import tpu as pltpu
from jax.sharding import PartitionSpec as P

NG = 128
KEPT = NG // 2
DEPTH = 6
ITERS = 3
F32 = jnp.float32
BF16 = jnp.bfloat16
MESH = pl.DeviceIdType.MESH

time_step = 0.25
energy_shift = 2.5
mixing_weight = 0.5
ridge_share = 0.1
ridge_floor = 0.01
density_scale = 8.0
bands_total = 32


def tables():
    frequency = np.arange(-(NG // 4), NG // 4, dtype=np.int32)
    positions = np.arange(NG, dtype=np.int32)
    phase = (positions[:, None] * frequency[None, :]) % NG
    angles = phase.astype(np.float32) * np.float32(2.0 * math.pi / NG)
    unit = np.float32(1.0 / math.sqrt(NG))
    cosine = (np.cos(angles) * unit).astype(ml_dtypes.bfloat16)
    sine = (np.sin(angles) * unit).astype(ml_dtypes.bfloat16)
    forward_z = np.concatenate(
        [np.concatenate([cosine, -sine], 1), np.concatenate([sine, cosine], 1)], 0
    )
    inverse_z = np.concatenate(
        [np.concatenate([cosine.T, sine.T], 1), np.concatenate([-sine.T, cosine.T], 1)], 0
    )
    stacked = np.concatenate([cosine.T, sine.T], 0)
    beside = np.concatenate([cosine, sine], 1)
    return np.concatenate(
        [forward_z, stacked, beside, inverse_z[:, :NG], inverse_z[:, NG:]], 0
    )


def dot(a, b):
    return jnp.dot(a, b, preferred_element_type=F32)


def kernel(
    occ, bands, ext, den, pden, pres, hden, hres, mats,
    out_d, out_r,
    mats_v, bands_v, ext_v, den_v, facg, facp, plane, rs, qs, psi,
    send_f, recv_f, stage, kin, send_b, recv_b, part, recv_d, row_s, rows, occ_s, occs,
    outs_s, outs_v,
    in_sems, pl_sems, pl_send, sf_sem, rf_sem, sb_sem, rb_sems, sd_sem, rd_sems,
    sr_sem, rr_sem, so_sem, ro_sem, sout_sems, rout_sems,
):
    g = lax.axis_index("band")
    i = lax.axis_index("grid")
    core = i % 2
    xy = i // 2
    half = g // 8
    zz = g % 8
    me = xy * 16 + g
    twin = i + 1 - 2 * core

    def remote(src, dst, ssem, rsem, dg, di):
        return pltpu.make_async_remote_copy(
            src_ref=src, dst_ref=dst, send_sem=ssem, recv_sem=rsem,
            device_id=(dg, di), device_id_type=MESH,
        )

    def drain(ref, sem):
        pltpu.make_async_copy(ref, ref, sem).wait()

    loads = [
        pltpu.make_async_copy(ext, ext_v, in_sems.at[0]),
        pltpu.make_async_copy(den, den_v, in_sems.at[1]),
        pltpu.make_async_copy(bands, bands_v, in_sems.at[2]),
        pltpu.make_async_copy(mats, mats_v, in_sems.at[3]),
    ]
    for load in loads:
        load.start()

    owner = core == half

    @pl.when(owner)
    def _():
        pieces = [
            (ext.at[zz], plane.at[0], 0), (den.at[zz], plane.at[1], 0),
            (pden.at[zz], plane.at[2], 0), (pres.at[zz], plane.at[3], 0),
            (hden.at[:, zz], rs.at[pl.ds(0, DEPTH - 1)], 1),
            (hres.at[:, zz], qs.at[pl.ds(0, DEPTH - 1)], 2),
        ]
        for src, dst, s in pieces:
            pltpu.make_async_copy(src, dst, pl_sems.at[s]).start()
            remote(src, dst, pl_send.at[s], pl_sems.at[s], g, twin).start()

    occ_row = jnp.full((1, NG), occ[core], F32)
    occ_s[...] = occ_row
    occs[g] = occ_row

    def send_occ(n, c):
        remote(occ_s, occs.at[g], so_sem, ro_sem, (g + n) % 16, i).start()
        return c

    lax.fori_loop(1, 16, send_occ, 0)

    lane = lax.broadcasted_iota(jnp.int32, (KEPT, NG), 1)
    sgn_f = jnp.where(lane < KEPT, 1.0, -1.0).astype(F32)
    sgn_i = -sgn_f
    fz = (lane % KEPT - NG // 4).astype(F32)
    fx = (lax.broadcasted_iota(jnp.int32, (KEPT, NG), 0) - NG // 4).astype(F32)
    quarter = NG / 4.0
    for r in range(8):
        fy = (8 * xy + r - NG // 4).astype(F32)
        kin[r] = jnp.exp((fx * fx + fy * fy + fz * fz) * (-time_step / (quarter * quarter)))

    def z_of(m):
        return (zz + 4 + (1 - 2 * (m % 2)) * ((m + 1) // 2)) % 8

    cols = [
        ((xy // 2 + dx) % 4) * 2 + (xy + dy) % 2 for dx in (2, 1, 3, 0) for dy in (1, 0)
    ]
    halves = [1 - half, half]

    wzf, fcs, ics = mats_v.at[pl.ds(0, 2 * NG)], mats_v.at[pl.ds(2 * NG, NG)], mats_v.at[pl.ds(3 * NG, NG)]
    wzi = mats_v.at[pl.ds(4 * NG, NG)], mats_v.at[pl.ds(5 * NG, NG)]

    def turned(a):
        return pltpu.roll(a, KEPT, 1)

    def pair_forward(x):
        pq = dot(fcs[...], x)
        return [
            pq[:KEPT, c : c + NG] + turned(pq[KEPT:, c : c + NG]) * sgn_f for c in (0, NG)
        ]

    def pair_inverse(d):
        both = [jnp.concatenate([v, turned(v) * sgn_i], axis=0).astype(BF16) for v in d]
        return dot(ics[...], jnp.concatenate(both, axis=1))

    def forward_zy(w):
        a = dot(w, wzf[...]).astype(BF16)
        b = pair_forward(jnp.concatenate([a[:NG], a[NG:]], axis=1))
        return [v.reshape(8, 8, NG).astype(BF16) for v in b]

    def send_tile(src, dst, ssem, rsem, dg, di, same=None):
        if same is None:
            remote(src, dst, ssem, rsem, dg, di).start()
            return

        @pl.when(same)
        def _():
            pltpu.make_async_copy(src, dst, rsem).start()

        @pl.when(jnp.logical_not(same))
        def _():
            remote(src, dst, ssem, rsem, dg, di).start()

    def spectral():
        drain(recv_f, rf_sem)
        stage[...] = recv_f[...].astype(F32).reshape(8 * NG, NG)
        for r in range(0, 8, 2):
            x = [stage[pl.ds(r + c, NG, stride=8), :].astype(BF16) for c in range(2)]
            b = pair_forward(jnp.concatenate(x, axis=1))
            y = pair_inverse([b[c] * kin[r + c] for c in range(2)])
            for c in range(2):
                stage[pl.ds(r + c, NG, stride=8), :] = y[:, c * NG : (c + 1) * NG]
        send_b[...] = stage[...].reshape(NG, 8, NG).astype(BF16)

        def send(m, carry):
            z = z_of(m)
            for h in range(2):
                dg = halves[h] * 8 + z
                for n, q in enumerate(cols):
                    send_tile(
                        send_b.at[q * 16 + dg], recv_b.at[g * 8 + xy], sb_sem, rb_sems.at[g],
                        dg, 2 * q + core, m == 7 if h == 1 and n == 7 else None,
                    )
            return carry

        lax.fori_loop(0, 8, send, 0)

    def backward(m, carry):
        z = z_of(m)
        ts = [halves[h] * 8 + z for h in range(2)]
        d = []
        for t in ts:
            tiles = recv_b.at[pl.ds(t * 8, 8)]
            drain(tiles, rb_sems.at[t])
            d.append(tiles[...].astype(F32).reshape(KEPT, NG))
        e = pair_inverse(d)
        e = jnp.concatenate([e[:, :NG], e[:, NG:]], axis=0).astype(BF16)
        re = dot(e, wzi[0][...]).astype(BF16)
        im = dot(e, wzi[1][...]).astype(BF16)
        total = part[...]
        for h, t in enumerate(ts):
            mine = slice(h * NG, (h + 1) * NG)
            psi[t, :, :NG] = re[mine]
            psi[t, :, NG:] = im[mine]
            wide_re, wide_im = re[mine].astype(F32), im[mine].astype(F32)
            total = total + occs[t] * (wide_re * wide_re + wide_im * wide_im)
        part[...] = total
        return carry

    gram = None
    for step in range(ITERS):
        if step == 0:
            for load in loads:
                load.wait()
            facg[...] = jnp.exp(-time_step * (ext_v[...] + den_v[...] - energy_shift))

            def make_forward(which, own):
                def forward(n, carry):
                    w = []
                    for c in range(2):
                        f = facg[2 * n + c]
                        w.append(jnp.concatenate(
                            [bands_v[p, which, 2 * n + c].astype(F32) * f for p in range(2)], axis=1
                        ).astype(BF16))
                    b = forward_zy(jnp.concatenate(w, axis=0))
                    for c in range(2):
                        at = own * 64 + (2 * n + c) * 8
                        send_f[pl.ds(at, 8)] = b[c]
                        for k, q in enumerate(cols):
                            src, dst = send_f.at[at + q], recv_f.at[8 * i + 2 * n + c]
                            if own and k == 7:
                                pltpu.make_async_copy(src, dst, rf_sem).start()
                            else:
                                send_tile(src, dst, sf_sem, rf_sem, g, 2 * q + which)
                    return carry

                return forward

            lax.fori_loop(0, 4, make_forward(1 - core, 0), 0)
            lax.fori_loop(0, 4, make_forward(core, 1), 0)
            drain(send_f.at[pl.ds(0, 120)], sf_sem)
        else:
            def forward(m, carry):
                z = z_of(m)
                f = facp[...]
                f = jnp.concatenate([f, f], axis=1)
                ts = [halves[h] * 8 + z for h in range(2)]
                w = jnp.concatenate([(psi[t].astype(F32) * f).astype(BF16) for t in ts], axis=0)
                b = forward_zy(w)
                for h, t in enumerate(ts):
                    send_f[pl.ds(t * 8, 8)] = b[h]
                    for n, q in enumerate(cols):
                        send_tile(
                            send_f.at[t * 8 + q], recv_f.at[me], sf_sem, rf_sem,
                            t, 2 * q + core, m == 7 if h == 1 and n == 7 else None,
                        )
                return carry

            lax.fori_loop(0, 8, forward, 0)
            drain(send_f.at[pl.ds(0, 127)], sf_sem)

        spectral()

        if step == 0:
            drain(plane, pl_sems.at[0])
            drain(rs.at[pl.ds(0, DEPTH - 1)], pl_sems.at[1])
            drain(qs.at[pl.ds(0, DEPTH - 1)], pl_sems.at[2])
            drain(occs.at[pl.ds(0, 15)], ro_sem)
            drain(occs.at[pl.ds(0, 15)], so_sem)

            @pl.when(owner)
            def _():
                drain(plane, pl_send.at[0])
                drain(rs.at[pl.ds(0, DEPTH - 1)], pl_send.at[1])
                drain(qs.at[pl.ds(0, DEPTH - 1)], pl_send.at[2])

        part[...] = jnp.zeros_like(part)
        lax.fori_loop(0, 8, backward, 0)
        drain(send_b.at[pl.ds(0, 127)], sb_sem)

        swap = remote(part, recv_d.at[step], sd_sem, rd_sems.at[step], g, twin)
        swap.start()
        swap.wait()
        rho_out = (part[...] + recv_d[step]) * (density_scale / bands_total)
        rho_in = plane[1]
        res = rho_out - rho_in
        newest = res - plane[3]
        rs[DEPTH - 1 + step] = rho_in - plane[2]
        qs[DEPTH - 1 + step] = newest

        def rows_of(a):
            return a.reshape(16, 8, NG)

        lanes = lax.broadcasted_iota(jnp.int32, (1, NG), 1)
        row = jnp.zeros((1, NG), F32)

        def put(row, at, a, b):
            total = jnp.sum(jnp.sum(rows_of(a * b), axis=0), axis=0, keepdims=True)
            return jnp.where(lanes == at, jnp.sum(total, axis=1, keepdims=True), row)

        for j in range(DEPTH):
            q = qs[step + j]
            row = put(row, j, q, newest)
            row = put(row, DEPTH + j, q, res)
        if step == 0:
            at = 2 * DEPTH
            for a in range(DEPTH - 1):
                for b in range(a + 1):
                    row = put(row, at, qs[a], qs[b])
                    at += 1
        row_s[...] = row
        rows[me] = row

        def send_row(m, carry):
            z = z_of(m)
            for h in range(2):
                for n, q in enumerate(cols):
                    copy = remote(
                        row_s, rows.at[me], sr_sem, rr_sem, halves[h] * 8 + z, 2 * q + core
                    )
                    if h == 1 and n == 7:
                        pl.when(m != 7)(copy.start)
                    else:
                        copy.start()
            return carry

        lax.fori_loop(0, 8, send_row, 0)

        def gather(value, which):
            outs_s[which] = value.astype(BF16)

            def send(m, carry):
                z = z_of(m)
                for h in range(2):
                    send_tile(
                        outs_s.at[which, pl.ds(pl.multiple_of(core * KEPT, KEPT), KEPT)],
                        outs_v.at[which, 2 * zz + core], sout_sems.at[which], rout_sems.at[which],
                        halves[h] * 8 + z, 2 * xy + half,
                        jnp.logical_and(m == 7, owner) if h == 1 else None,
                    )
                return carry

            lax.fori_loop(0, 8, send, 0)

        if step == ITERS - 1:
            gather(res, 1)

        drain(rows.at[pl.ds(0, 127)], rr_sem)
        drain(rows.at[pl.ds(0, 127)], sr_sem)
        sums = jnp.sum(rows[...], axis=0) * (1.0 / (NG * NG * NG))

        def splat(at):
            return jnp.broadcast_to(sums[:, at : at + 1], (8, NG))

        border = [splat(j) for j in range(DEPTH)]
        right = [splat(DEPTH + j) for j in range(DEPTH)]
        if step == 0:
            at = 2 * DEPTH
            gram = []
            for a in range(DEPTH - 1):
                gram.append([splat(at + b) for b in range(a + 1)])
                at += a + 1
        else:
            gram = [[gram[a][b] for b in range(1, a + 1)] for a in range(1, DEPTH)]
        gram.append(border)
        trace = gram[0][0]
        for j in range(1, DEPTH):
            trace = trace + gram[j][j]
        ridge = trace * (ridge_share / DEPTH) + ridge_floor
        low = [[None] * DEPTH for _ in range(DEPTH)]
        scaled = [[None] * DEPTH for _ in range(DEPTH)]
        inverse = [None] * DEPTH
        for c in range(DEPTH):
            value = gram[c][c] + ridge
            for k in range(c):
                value = value - scaled[c][k] * low[c][k]
            inverse[c] = 1.0 / value
            for r in range(c + 1, DEPTH):
                value = gram[r][c]
                for k in range(c):
                    value = value - scaled[r][k] * low[c][k]
                scaled[r][c] = value
                low[r][c] = value * inverse[c]
        middle = []
        for r in range(DEPTH):
            value = right[r]
            for k in range(r):
                value = value - low[r][k] * middle[k]
            middle.append(value)
        coeffs = [None] * DEPTH
        for r in reversed(range(DEPTH)):
            value = middle[r] * inverse[r]
            for k in range(r + 1, DEPTH):
                value = value - low[k][r] * coeffs[k]
            coeffs[r] = value
        mixed = rows_of(rho_in + mixing_weight * res)
        for j in range(DEPTH):
            mixed = mixed - coeffs[j][None] * rows_of(rs[step + j] + mixing_weight * qs[step + j])
        rho = mixed.reshape(NG, NG)
        if step < ITERS - 1:
            plane[2] = rho_in
            plane[3] = res
            plane[1] = rho
            facp[...] = jnp.exp(-time_step * (plane[0] + rho - energy_shift))
        else:
            gather(rho, 0)
            for which, out in ((1, out_r), (0, out_d)):
                drain(outs_v.at[which], rout_sems.at[which])
                out[...] = outs_v[which].astype(F32).reshape(8, NG, NG)

                @pl.when(owner)
                def _():
                    drain(outs_v.at[which, pl.ds(0, 15)], sout_sems.at[which])

                @pl.when(jnp.logical_not(owner))
                def _():
                    drain(outs_v.at[which], sout_sems.at[which])


def local(bands, occupations, external, density_in, prev_density, prev_residual, hist_density, hist_residual):
    slab = external.shape
    hbm = pl.BlockSpec(memory_space=pltpu.HBM)
    vmem = pl.BlockSpec(memory_space=pltpu.VMEM)
    smem = pl.BlockSpec(memory_space=pltpu.SMEM)
    dma = pltpu.SemaphoreType.DMA
    out = jax.ShapeDtypeStruct(slab, F32)
    return pl.pallas_call(
        kernel,
        out_shape=(out, out),
        in_specs=[smem] + [hbm] * 8,
        out_specs=(vmem, vmem),
        scratch_shapes=[
            pltpu.VMEM((6 * NG, NG), BF16),
            pltpu.VMEM(bands.shape, BF16),
            pltpu.VMEM(slab, F32),
            pltpu.VMEM(slab, F32),
            pltpu.VMEM(slab, F32),
            pltpu.VMEM((NG, NG), F32),
            pltpu.VMEM((4, NG, NG), F32),
            pltpu.VMEM((DEPTH - 1 + ITERS, NG, NG), F32),
            pltpu.VMEM((DEPTH - 1 + ITERS, NG, NG), F32),
            pltpu.VMEM((16, NG, 2 * NG), BF16),
            pltpu.VMEM((128, 8, NG), BF16),
            pltpu.VMEM((128, 8, NG), BF16),
            pltpu.VMEM((8 * NG, NG), F32),
            pltpu.VMEM((8, KEPT, NG), F32),
            pltpu.VMEM((128, 8, NG), BF16),
            pltpu.VMEM((128, 8, NG), BF16),
            pltpu.VMEM((NG, NG), F32),
            pltpu.VMEM((ITERS, NG, NG), F32),
            pltpu.VMEM((1, NG), F32),
            pltpu.VMEM((128, 1, NG), F32),
            pltpu.VMEM((1, NG), F32),
            pltpu.VMEM((16, 1, NG), F32),
            pltpu.VMEM((2, NG, NG), BF16),
            pltpu.VMEM((2, 16, KEPT, NG), BF16),
            dma((4,)), dma((3,)), dma((3,)),
            dma(()), dma(()), dma(()), dma((16,)), dma(()), dma((ITERS,)),
            dma(()), dma(()), dma(()), dma(()), dma((2,)), dma((2,)),
        ],
        compiler_params=pltpu.CompilerParams(
            has_side_effects=True, vmem_limit_bytes=67043328
        ),
        name="scf",
    )(
        occupations, bands, external, density_in, prev_density, prev_residual,
        hist_density, hist_residual, jnp.asarray(tables()),
    )


def solution(mesh):
    placed = (
        P(None, "band", "grid", None, None),
        P("band"),
        P("grid", None, None),
        P("grid", None, None),
        P("grid", None, None),
        P("grid", None, None),
        P(None, "grid", None, None),
        P(None, "grid", None, None),
    )
    return jax.shard_map(
        local,
        mesh=mesh,
        in_specs=placed,
        out_specs=(P("grid", None, None), P("grid", None, None)),
        check_vma=False,
    )
```

```python
import math

import jax
import jax.numpy as jnp
import ml_dtypes
import numpy as np
from jax import lax
from jax.experimental import pallas as pl
from jax.experimental.pallas import tpu as pltpu
from jax.sharding import PartitionSpec as P

NG = 128
KEPT = NG // 2
DEPTH = 6
ITERS = 3
PER = 4
F32 = jnp.float32
BF16 = jnp.bfloat16
MESH = pl.DeviceIdType.MESH

time_step = 0.25
energy_shift = 2.5
mixing_weight = 0.5
ridge_share = 0.1
ridge_floor = 0.01
density_scale = 8.0
bands_total = 32


def tables():
    frequency = np.arange(-(NG // 4), NG // 4, dtype=np.int32)
    positions = np.arange(NG, dtype=np.int32)
    phase = (positions[:, None] * frequency[None, :]) % NG
    angles = phase.astype(np.float32) * np.float32(2.0 * math.pi / NG)
    unit = np.float32(1.0 / math.sqrt(NG))
    cosine = (np.cos(angles) * unit).astype(ml_dtypes.bfloat16)
    sine = (np.sin(angles) * unit).astype(ml_dtypes.bfloat16)
    forward_z = np.concatenate(
        [np.concatenate([cosine, -sine], 1), np.concatenate([sine, cosine], 1)], 0
    )
    inverse_z = np.concatenate(
        [np.concatenate([cosine.T, sine.T], 1), np.concatenate([-sine.T, cosine.T], 1)], 0
    )
    stacked = np.concatenate([cosine.T, sine.T], 0)
    beside = np.concatenate([cosine, sine], 1)
    return np.concatenate(
        [forward_z, stacked, beside, inverse_z[:, :NG], inverse_z[:, NG:]], 0
    )


def dot(a, b):
    return jnp.dot(a, b, preferred_element_type=F32)


def kernel(
    occ, bands, ext, den, pden, pres, hden, hres, mats,
    out_d, out_r,
    mats_v, bands_v, ext_v, den_v, facg, facp, plane, rs, qs, psi,
    send_f, recv_f, stage, kin, send_b, recv_b, part, recv_d, row_s, rows, occ_s, occs,
    outs_s,
    in_sems, pl_sems, pl_send, sf_sem, rf_sem, sb_sem, rb_sems, sd_sem, rd_sems,
    sr_sem, rr_sem, so_sem, ro_sem, sout_sems, rout_sems,
):
    outs_v = (out_d, out_r)
    g = lax.axis_index("band")
    i = lax.axis_index("grid")
    core = i % 2
    xy = i // 2
    half = g // 8
    zz = g % 8
    me = xy * 16 + g
    twin = i + 1 - 2 * core
    owner = core == half

    def remote(src, dst, ssem, rsem, dg, di):
        return pltpu.make_async_remote_copy(
            src_ref=src, dst_ref=dst, send_sem=ssem, recv_sem=rsem,
            device_id=(dg, di), device_id_type=MESH,
        )

    def drain(ref, sem):
        pltpu.make_async_copy(ref, ref, sem).wait()

    def z_of(m):
        return (zz + 4 + (1 - 2 * (m % 2)) * ((m + 1) // 2)) % 8

    def col_of(n):
        k = n // 2
        dx = 2 + (1 - 2 * (k % 2)) * ((k + 1) // 2)
        return ((xy // 2 + dx) % 4) * 2 + (xy + 1 - n % 2) % 2

    halves = [1 - half, half]
    rings = [halves[h] * 8 + z_of(m) for m in range(8) for h in range(2)]

    def everyone(start):
        def column(n, carry):
            q = col_of(n)
            for at, dg in enumerate(rings):
                start(dg, q, n == 7 if at == 15 else None)
            return carry

        lax.fori_loop(0, 8, column, 0)


    barrier = pltpu.get_barrier_semaphore()

    def hello(dg, di):
        pl.semaphore_signal(barrier, inc=1, device_id=(dg, di), device_id_type=MESH)

    def greet(dg, q, same):
        if same is None:
            hello(dg, 2 * q + core)
        else:
            pl.when(jnp.logical_not(same))(lambda: hello(dg, 2 * q + core))

    everyone(greet)
    for dg in rings:
        hello(dg, twin)

    def greet_column(n, carry):
        hello(g, 2 * col_of(n) + 1 - core)
        return carry

    lax.fori_loop(0, 7, greet_column, 0)

    loads = [
        pltpu.make_async_copy(ext, ext_v, in_sems.at[0]),
        pltpu.make_async_copy(den, den_v, in_sems.at[1]),
        pltpu.make_async_copy(bands, bands_v, in_sems.at[2]),
        pltpu.make_async_copy(mats, mats_v, in_sems.at[3]),
    ]
    for load in loads:
        load.start()

    lane = lax.broadcasted_iota(jnp.int32, (KEPT, NG), 1)
    sgn_f = jnp.where(lane < KEPT, 1.0, -1.0).astype(F32)
    sgn_i = -sgn_f
    fz = (lane % KEPT - NG // 4).astype(F32)
    fx = (lax.broadcasted_iota(jnp.int32, (KEPT, NG), 0) - NG // 4).astype(F32)
    quarter = NG / 4.0
    for r in range(8):
        fy = (8 * xy + r - NG // 4).astype(F32)
        kin[r] = jnp.exp((fx * fx + fy * fy + fz * fz) * (-time_step / (quarter * quarter)))

    wzf, fcs, ics = mats_v.at[pl.ds(0, 2 * NG)], mats_v.at[pl.ds(2 * NG, NG)], mats_v.at[pl.ds(3 * NG, NG)]
    wzi = mats_v.at[pl.ds(4 * NG, NG)], mats_v.at[pl.ds(5 * NG, NG)]

    def turned(a):
        return pltpu.roll(a, KEPT, 1)

    def pair_forward(x):
        pq = dot(fcs[...], x)
        return [
            pq[:KEPT, c : c + NG] + turned(pq[KEPT:, c : c + NG]) * sgn_f for c in (0, NG)
        ]

    def pair_inverse(d):
        both = [jnp.concatenate([v, turned(v) * sgn_i], axis=0).astype(BF16) for v in d]
        return dot(ics[...], jnp.concatenate(both, axis=1))

    def forward_zy(w):
        a = dot(w, wzf[...]).astype(BF16)
        out = []
        for at in range(0, w.shape[0], 2 * NG):
            b = pair_forward(jnp.concatenate([a[at : at + NG], a[at + NG : at + 2 * NG]], axis=1))
            out += [v.reshape(8, 8, NG).astype(BF16) for v in b]
        return out

    def send_tile(src, dst, ssem, rsem, dg, di, same=None):
        if same is None:
            remote(src, dst, ssem, rsem, dg, di).start()
            return

        @pl.when(same)
        def _():
            pltpu.make_async_copy(src, dst, rsem).start()

        @pl.when(jnp.logical_not(same))
        def _():
            remote(src, dst, ssem, rsem, dg, di).start()

    def spectral():
        drain(recv_f, rf_sem)
        stage[...] = recv_f[...].astype(F32).reshape(8 * NG, NG)
        for r in range(0, 8, 2):
            x = [stage[pl.ds(r + c, NG, stride=8), :].astype(BF16) for c in range(2)]
            b = pair_forward(jnp.concatenate(x, axis=1))
            y = pair_inverse([b[c] * kin[r + c] for c in range(2)])
            for c in range(2):
                stage[pl.ds(r + c, NG, stride=8), :] = y[:, c * NG : (c + 1) * NG]
        send_b[...] = stage[...].reshape(NG, 8, NG).astype(BF16)

        everyone(lambda dg, q, same: send_tile(
            send_b.at[q * 16 + dg], recv_b.at[g * 8 + xy], sb_sem, rb_sems.at[g],
            dg, 2 * q + core, same,
        ))

    def bands_of(n):
        return [halves[h] * 8 + z_of(n * PER + e) for e in range(PER) for h in range(2)]

    def backward(n, carry):
        ts = bands_of(n)
        d = []
        for t in ts:
            tiles = recv_b.at[pl.ds(t * 8, 8)]
            drain(tiles, rb_sems.at[t])
            d.append(tiles[...].astype(F32).reshape(KEPT, NG))
        e = []
        for at in range(0, len(ts), 2):
            both = pair_inverse(d[at : at + 2])
            e += [both[:, :NG], both[:, NG:]]
        e = jnp.concatenate(e, axis=0).astype(BF16)
        re = dot(e, wzi[0][...]).astype(BF16)
        im = dot(e, wzi[1][...]).astype(BF16)
        total = part[...]
        for h, t in enumerate(ts):
            mine = slice(h * NG, (h + 1) * NG)
            psi[t, :, :NG] = re[mine]
            psi[t, :, NG:] = im[mine]
            wide_re, wide_im = re[mine].astype(F32), im[mine].astype(F32)
            total = total + occs[t] * (wide_re * wide_re + wide_im * wide_im)
        part[...] = total
        return carry

    gram = None
    for step in range(ITERS):
        if step == 0:
            for load in loads:
                load.wait()
            facg[...] = jnp.exp(-time_step * (ext_v[...] + den_v[...] - energy_shift))

            def forward(n, carry):
                w = []
                for c in range(2 * PER):
                    at = n * 2 * PER + c
                    f = facg[at % 8]
                    w.append(jnp.concatenate(
                        [bands_v[p, at // 8, at % 8].astype(F32) * f for p in range(2)], axis=1
                    ).astype(BF16))
                for c, b in enumerate(forward_zy(jnp.concatenate(w, axis=0))):
                    send_f[pl.ds((n * 2 * PER + c) * 8, 8)] = b
                return carry

            lax.fori_loop(0, 8 // PER, forward, 0)
            pl.semaphore_wait(barrier, 150)
            columns = [col_of(n) for n in range(8)]

            def first_sends(n, carry):
                which, j = n // 8, n % 8
                for k, q in enumerate(columns):
                    send_tile(
                        send_f.at[n * 8 + q], recv_f.at[8 * i + j], sf_sem, rf_sem, g, 2 * q + which,
                        which == core if k == 7 else None,
                    )
                return carry

            lax.fori_loop(0, 16, first_sends, 0)


            @pl.when(owner)
            def _():
                pieces = [
                    (ext.at[zz], plane.at[0], 0), (den.at[zz], plane.at[1], 0),
                    (pden.at[zz], plane.at[2], 0), (pres.at[zz], plane.at[3], 0),
                    (hden.at[:, zz], rs.at[pl.ds(0, DEPTH - 1)], 1),
                    (hres.at[:, zz], qs.at[pl.ds(0, DEPTH - 1)], 2),
                ]
                for src, dst, s in pieces:
                    pltpu.make_async_copy(src, dst, pl_sems.at[s]).start()
                    remote(src, dst, pl_send.at[s], pl_sems.at[s], g, twin).start()

            occ_row = jnp.full((1, NG), occ[core], F32)
            occ_s[...] = occ_row
            occs[g] = occ_row

            def send_occ(n, c):
                remote(occ_s, occs.at[g], so_sem, ro_sem, (g + n) % 16, i).start()
                return c

            lax.fori_loop(1, 16, send_occ, 0)

        else:
            def forward(n, carry):
                ts = bands_of(n)
                f = facp[...]
                f = jnp.concatenate([f, f], axis=1)
                w = jnp.concatenate([(psi[t].astype(F32) * f).astype(BF16) for t in ts], axis=0)
                for t, b in zip(ts, forward_zy(w)):
                    send_f[pl.ds(t * 8, 8)] = b
                return carry

            lax.fori_loop(0, 8 // PER, forward, 0)
            everyone(lambda dg, q, same: send_tile(
                send_f.at[dg * 8 + q], recv_f.at[me], sf_sem, rf_sem, dg, 2 * q + core, same,
            ))

        spectral()
        drain(send_f.at[pl.ds(0, 120 if step == 0 else 127)], sf_sem)

        if step == 0:
            drain(plane, pl_sems.at[0])
            drain(rs.at[pl.ds(0, DEPTH - 1)], pl_sems.at[1])
            drain(qs.at[pl.ds(0, DEPTH - 1)], pl_sems.at[2])
            drain(occs.at[pl.ds(0, 15)], ro_sem)
            drain(occs.at[pl.ds(0, 15)], so_sem)

            @pl.when(owner)
            def _():
                drain(plane, pl_send.at[0])
                drain(rs.at[pl.ds(0, DEPTH - 1)], pl_send.at[1])
                drain(qs.at[pl.ds(0, DEPTH - 1)], pl_send.at[2])

        part[...] = jnp.zeros_like(part)
        lax.fori_loop(0, 8 // PER, backward, 0)

        swap = remote(part, recv_d.at[step], sd_sem, rd_sems.at[step], g, twin)
        swap.start()
        swap.wait_recv()
        rho_out = (part[...] + recv_d[step]) * (density_scale / bands_total)
        rho_in = plane[1]
        res = rho_out - rho_in
        newest = res - plane[3]
        rs[DEPTH - 1 + step] = rho_in - plane[2]
        qs[DEPTH - 1 + step] = newest

        def rows_of(a):
            return a.reshape(16, 8, NG)

        lanes = lax.broadcasted_iota(jnp.int32, (1, NG), 1)
        row = jnp.zeros((1, NG), F32)

        def put(row, at, a, b):
            total = jnp.sum(jnp.sum(rows_of(a * b), axis=0), axis=0, keepdims=True)
            return jnp.where(lanes == at, jnp.sum(total, axis=1, keepdims=True), row)

        for j in range(DEPTH):
            q = qs[step + j]
            row = put(row, j, q, newest)
            row = put(row, DEPTH + j, q, res)
        if step == 0:
            at = 2 * DEPTH
            for a in range(DEPTH - 1):
                for b in range(a + 1):
                    row = put(row, at, qs[a], qs[b])
                    at += 1
        row_s[...] = row
        rows[me] = row

        def send_row(dg, q, same):
            copy = remote(row_s, rows.at[me], sr_sem, rr_sem, dg, 2 * q + core)
            if same is None:
                copy.start()
            else:
                pl.when(jnp.logical_not(same))(copy.start)

        everyone(send_row)

        def gather(value, which):
            outs_s[which] = value.astype(BF16)

            def send(m, carry):
                z = z_of(m)
                for h in range(2):
                    send_tile(
                        outs_s.at[which, pl.ds(pl.multiple_of(core * KEPT, KEPT), KEPT)],
                        outs_v[which].at[2 * zz + core], sout_sems.at[which], rout_sems.at[which],
                        halves[h] * 8 + z, 2 * xy + half,
                        jnp.logical_and(m == 7, owner) if h == 1 else None,
                    )
                return carry

            lax.fori_loop(0, 8, send, 0)

        if step == ITERS - 1:
            gather(res, 1)

        swap.wait_send()
        drain(rows.at[pl.ds(0, 127)], rr_sem)
        drain(rows.at[pl.ds(0, 127)], sr_sem)
        drain(send_b.at[pl.ds(0, 127)], sb_sem)
        sums = jnp.sum(rows[...], axis=0) * (1.0 / (NG * NG * NG))

        def splat(at):
            return jnp.broadcast_to(sums[:, at : at + 1], (8, NG))

        border = [splat(j) for j in range(DEPTH)]
        right = [splat(DEPTH + j) for j in range(DEPTH)]
        if step == 0:
            at = 2 * DEPTH
            gram = []
            for a in range(DEPTH - 1):
                gram.append([splat(at + b) for b in range(a + 1)])
                at += a + 1
        else:
            gram = [[gram[a][b] for b in range(1, a + 1)] for a in range(1, DEPTH)]
        gram.append(border)
        trace = gram[0][0]
        for j in range(1, DEPTH):
            trace = trace + gram[j][j]
        ridge = trace * (ridge_share / DEPTH) + ridge_floor
        low = [[None] * DEPTH for _ in range(DEPTH)]
        scaled = [[None] * DEPTH for _ in range(DEPTH)]
        inverse = [None] * DEPTH
        for c in range(DEPTH):
            value = gram[c][c] + ridge
            for k in range(c):
                value = value - scaled[c][k] * low[c][k]
            inverse[c] = 1.0 / value
            for r in range(c + 1, DEPTH):
                value = gram[r][c]
                for k in range(c):
                    value = value - scaled[r][k] * low[c][k]
                scaled[r][c] = value
                low[r][c] = value * inverse[c]
        middle = []
        for r in range(DEPTH):
            value = right[r]
            for k in range(r):
                value = value - low[r][k] * middle[k]
            middle.append(value)
        coeffs = [None] * DEPTH
        for r in reversed(range(DEPTH)):
            value = middle[r] * inverse[r]
            for k in range(r + 1, DEPTH):
                value = value - low[k][r] * coeffs[k]
            coeffs[r] = value
        mixed = rows_of(rho_in + mixing_weight * res)
        for j in range(DEPTH):
            mixed = mixed - coeffs[j][None] * rows_of(rs[step + j] + mixing_weight * qs[step + j])
        rho = mixed.reshape(NG, NG)
        if step < ITERS - 1:
            plane[2] = rho_in
            plane[3] = res
            plane[1] = rho
            facp[...] = jnp.exp(-time_step * (plane[0] + rho - energy_shift))
        else:
            gather(rho, 0)
            for which in (1, 0):
                drain(outs_v[which], rout_sems.at[which])

                @pl.when(owner)
                def _():
                    drain(outs_v[which].at[pl.ds(0, 15)], sout_sems.at[which])

                @pl.when(jnp.logical_not(owner))
                def _():
                    drain(outs_v[which], sout_sems.at[which])


def local(bands, occupations, external, density_in, prev_density, prev_residual, hist_density, hist_residual):
    slab = external.shape
    hbm = pl.BlockSpec(memory_space=pltpu.HBM)
    smem = pl.BlockSpec(memory_space=pltpu.SMEM)
    dma = pltpu.SemaphoreType.DMA
    both = pl.pallas_call(
        kernel,
        out_shape=[jax.ShapeDtypeStruct((16, KEPT, NG), BF16)] * 2,
        in_specs=[smem] + [hbm] * 8,
        out_specs=[hbm] * 2,
        scratch_shapes=[
            pltpu.VMEM((6 * NG, NG), BF16),
            pltpu.VMEM(bands.shape, BF16),
            pltpu.VMEM(slab, F32),
            pltpu.VMEM(slab, F32),
            pltpu.VMEM(slab, F32),
            pltpu.VMEM((NG, NG), F32),
            pltpu.VMEM((4, NG, NG), F32),
            pltpu.VMEM((DEPTH - 1 + ITERS, NG, NG), F32),
            pltpu.VMEM((DEPTH - 1 + ITERS, NG, NG), F32),
            pltpu.VMEM((16, NG, 2 * NG), BF16),
            pltpu.VMEM((128, 8, NG), BF16),
            pltpu.VMEM((128, 8, NG), BF16),
            pltpu.VMEM((8 * NG, NG), F32),
            pltpu.VMEM((8, KEPT, NG), F32),
            pltpu.VMEM((128, 8, NG), BF16),
            pltpu.VMEM((128, 8, NG), BF16),
            pltpu.VMEM((NG, NG), F32),
            pltpu.VMEM((ITERS, NG, NG), F32),
            pltpu.VMEM((1, NG), F32),
            pltpu.VMEM((128, 1, NG), F32),
            pltpu.VMEM((1, NG), F32),
            pltpu.VMEM((16, 1, NG), F32),
            pltpu.VMEM((2, NG, NG), BF16),
            dma((4,)), dma((3,)), dma((3,)),
            dma(()), dma(()), dma(()), dma((16,)), dma(()), dma((ITERS,)),
            dma(()), dma(()), dma(()), dma(()), dma((2,)), dma((2,)),
        ],
        compiler_params=pltpu.CompilerParams(
            has_side_effects=True, collective_id=0, vmem_limit_bytes=67043328
        ),
        name="scf",
    )(
        occupations, bands, external, density_in, prev_density, prev_residual,
        hist_density, hist_residual, jnp.asarray(tables()),
    )
    return tuple(half.reshape(slab).astype(F32) for half in both)


def solution(mesh):
    placed = (
        P(None, "band", "grid", None, None),
        P("band"),
        P("grid", None, None),
        P("grid", None, None),
        P("grid", None, None),
        P("grid", None, None),
        P(None, "grid", None, None),
        P(None, "grid", None, None),
    )
    return jax.shard_map(
        local,
        mesh=mesh,
        in_specs=placed,
        out_specs=(P("grid", None, None), P("grid", None, None)),
        check_vma=False,
    )
```

```python
import math

import jax
import jax.numpy as jnp
import ml_dtypes
import numpy as np
from jax import lax
from jax.experimental import pallas as pl
from jax.experimental.pallas import tpu as pltpu
from jax.sharding import PartitionSpec as P

NG = 128
KEPT = NG // 2
DEPTH = 6
ITERS = 3
PER = 4
F32 = jnp.float32
BF16 = jnp.bfloat16
MESH = pl.DeviceIdType.MESH

time_step = 0.25
energy_shift = 2.5
mixing_weight = 0.5
ridge_share = 0.1
ridge_floor = 0.01
density_scale = 8.0
bands_total = 32


def tables():
    frequency = np.arange(-(NG // 4), NG // 4, dtype=np.int32)
    positions = np.arange(NG, dtype=np.int32)
    phase = (positions[:, None] * frequency[None, :]) % NG
    angles = phase.astype(np.float32) * np.float32(2.0 * math.pi / NG)
    unit = np.float32(1.0 / math.sqrt(NG))
    cosine = (np.cos(angles) * unit).astype(ml_dtypes.bfloat16)
    sine = (np.sin(angles) * unit).astype(ml_dtypes.bfloat16)
    forward_z = np.concatenate(
        [np.concatenate([cosine, -sine], 1), np.concatenate([sine, cosine], 1)], 0
    )
    inverse_z = np.concatenate(
        [np.concatenate([cosine.T, sine.T], 1), np.concatenate([-sine.T, cosine.T], 1)], 0
    )
    stacked = np.concatenate([cosine.T, sine.T], 0)
    beside = np.concatenate([cosine, sine], 1)
    return np.concatenate(
        [forward_z, stacked, beside, inverse_z[:, :NG], inverse_z[:, NG:]], 0
    )


def dot(a, b):
    return jnp.dot(a, b, preferred_element_type=F32)


def kernel(
    occ, bands, ext, den, pden, pres, hden, hres, mats,
    out_d, out_r,
    mats_v, bands_v, ext_v, den_v, facg, facp, plane, rs, qs, psi,
    send_f, recv_f, stage, kin, send_b, recv_b, part, recv_d, row_s, rows, occ_s, occs,
    outs_s, res_v, den_s, rslab, qslab, pden_v, pres_v, coef_v,
    in_sems, pl_sems, pl_send, sf_sem, rf_sem, sb_sem, rb_sems, sd_sem, rd_sems,
    sr_sem, rr_sem, so_sem, ro_sem, sout_sems, rout_sems, late_sems, fin_sems,
):
    g = lax.axis_index("band")
    i = lax.axis_index("grid")
    core = i % 2
    xy = i // 2
    half = g // 8
    zz = g % 8
    me = xy * 16 + g
    twin = i + 1 - 2 * core
    owner = core == half

    def remote(src, dst, ssem, rsem, dg, di):
        return pltpu.make_async_remote_copy(
            src_ref=src, dst_ref=dst, send_sem=ssem, recv_sem=rsem,
            device_id=(dg, di), device_id_type=MESH,
        )

    def drain(ref, sem):
        pltpu.make_async_copy(ref, ref, sem).wait()

    loads = [
        pltpu.make_async_copy(ext, ext_v, in_sems.at[0]),
        pltpu.make_async_copy(den, den_v, in_sems.at[1]),
        pltpu.make_async_copy(bands, bands_v, in_sems.at[2]),
        pltpu.make_async_copy(mats, mats_v, in_sems.at[3]),
    ]
    for load in loads:
        load.start()
    late = [
        pltpu.make_async_copy(hden, rslab.at[pl.ds(0, DEPTH - 1)], late_sems.at[0]),
        pltpu.make_async_copy(hres, qslab.at[pl.ds(0, DEPTH - 1)], late_sems.at[1]),
        pltpu.make_async_copy(pden, pden_v, late_sems.at[2]),
        pltpu.make_async_copy(pres, pres_v, late_sems.at[3]),
    ]

    def z_of(m):
        return (zz + 4 + (1 - 2 * (m % 2)) * ((m + 1) // 2)) % 8

    def col_of(n):
        k = n // 2
        dx = 2 + (1 - 2 * (k % 2)) * ((k + 1) // 2)
        return ((xy // 2 + dx) % 4) * 2 + (xy + 1 - n % 2) % 2

    halves = [1 - half, half]
    rings = [halves[h] * 8 + z_of(m) for m in range(8) for h in range(2)]

    def everyone(start):
        def column(n, carry):
            q = col_of(n)
            for at, dg in enumerate(rings):
                start(dg, q, n == 7 if at == 15 else None)
            return carry

        lax.fori_loop(0, 8, column, 0)


    barrier = pltpu.get_barrier_semaphore()

    def hello(dg, di):
        pl.semaphore_signal(barrier, inc=1, device_id=(dg, di), device_id_type=MESH)

    def greet(dg, q, same):
        if same is None:
            hello(dg, 2 * q + core)
        else:
            pl.when(jnp.logical_not(same))(lambda: hello(dg, 2 * q + core))

    everyone(greet)
    for dg in rings:
        hello(dg, twin)

    def greet_column(n, carry):
        hello(g, 2 * col_of(n) + 1 - core)
        return carry

    lax.fori_loop(0, 7, greet_column, 0)

    lane = lax.broadcasted_iota(jnp.int32, (KEPT, NG), 1)
    sgn_f = jnp.where(lane < KEPT, 1.0, -1.0).astype(F32)
    sgn_i = -sgn_f
    fz = (lane % KEPT - NG // 4).astype(F32)
    fx = (lax.broadcasted_iota(jnp.int32, (KEPT, NG), 0) - NG // 4).astype(F32)
    quarter = NG / 4.0
    for r in range(8):
        fy = (8 * xy + r - NG // 4).astype(F32)
        kin[r] = jnp.exp((fx * fx + fy * fy + fz * fz) * (-time_step / (quarter * quarter)))

    wzf, fcs, ics = mats_v.at[pl.ds(0, 2 * NG)], mats_v.at[pl.ds(2 * NG, NG)], mats_v.at[pl.ds(3 * NG, NG)]
    wzi = mats_v.at[pl.ds(4 * NG, NG)], mats_v.at[pl.ds(5 * NG, NG)]

    def turned(a):
        return pltpu.roll(a, KEPT, 1)

    def pair_forward(x):
        pq = dot(fcs[...], x)
        return [
            pq[:KEPT, c : c + NG] + turned(pq[KEPT:, c : c + NG]) * sgn_f for c in (0, NG)
        ]

    def pair_inverse(d):
        both = [jnp.concatenate([v, turned(v) * sgn_i], axis=0).astype(BF16) for v in d]
        return dot(ics[...], jnp.concatenate(both, axis=1))

    def forward_zy(w):
        a = dot(w, wzf[...]).astype(BF16)
        out = []
        for at in range(0, w.shape[0], 2 * NG):
            b = pair_forward(jnp.concatenate([a[at : at + NG], a[at + NG : at + 2 * NG]], axis=1))
            out += [v.reshape(8, 8, NG).astype(BF16) for v in b]
        return out

    def send_tile(src, dst, ssem, rsem, dg, di, same=None):
        if same is None:
            remote(src, dst, ssem, rsem, dg, di).start()
            return

        @pl.when(same)
        def _():
            pltpu.make_async_copy(src, dst, rsem).start()

        @pl.when(jnp.logical_not(same))
        def _():
            remote(src, dst, ssem, rsem, dg, di).start()

    def spectral():
        drain(recv_f, rf_sem)
        stage[...] = recv_f[...].astype(F32).reshape(8 * NG, NG)
        for r in range(0, 8, 2):
            x = [stage[pl.ds(r + c, NG, stride=8), :].astype(BF16) for c in range(2)]
            b = pair_forward(jnp.concatenate(x, axis=1))
            y = pair_inverse([b[c] * kin[r + c] for c in range(2)])
            for c in range(2):
                stage[pl.ds(r + c, NG, stride=8), :] = y[:, c * NG : (c + 1) * NG]
        send_b[...] = stage[...].reshape(NG, 8, NG).astype(BF16)

        everyone(lambda dg, q, same: send_tile(
            send_b.at[q * 16 + dg], recv_b.at[g * 8 + xy], sb_sem, rb_sems.at[g],
            dg, 2 * q + core, same,
        ))

    def bands_of(n):
        return [halves[h] * 8 + z_of(n * PER + e) for e in range(PER) for h in range(2)]

    def backward(n, carry):
        ts = bands_of(n)
        d = []
        for t in ts:
            tiles = recv_b.at[pl.ds(t * 8, 8)]
            drain(tiles, rb_sems.at[t])
            d.append(tiles[...].astype(F32).reshape(KEPT, NG))
        e = []
        for at in range(0, len(ts), 2):
            both = pair_inverse(d[at : at + 2])
            e += [both[:, :NG], both[:, NG:]]
        e = jnp.concatenate(e, axis=0).astype(BF16)
        re = dot(e, wzi[0][...]).astype(BF16)
        im = dot(e, wzi[1][...]).astype(BF16)
        total = part[...]
        for h, t in enumerate(ts):
            mine = slice(h * NG, (h + 1) * NG)
            psi[t, :, :NG] = re[mine]
            psi[t, :, NG:] = im[mine]
            wide_re, wide_im = re[mine].astype(F32), im[mine].astype(F32)
            total = total + occs[t] * (wide_re * wide_re + wide_im * wide_im)
        part[...] = total
        return carry

    def rows_of(a):
        return a.reshape(16, 8, NG)

    def slab_update(done):
        drain(res_v.at[done], rout_sems.at[done])
        last = done == ITERS - 1
        if last:
            keep = pltpu.make_async_copy(res_v.at[done], out_r, fin_sems.at[1])
            keep.start()

        def one_plane(j, carry):
            here = res_v[done, pl.ds(2 * j, 2)].astype(F32).reshape(NG, NG)
            inside = den_v[j]
            fresh_r, fresh_q = inside - pden_v[j], here - pres_v[j]
            mixed = rows_of(inside + mixing_weight * here)
            for k in range(DEPTH):
                r = rslab[done + k, j] if k < DEPTH - 1 else fresh_r
                q = qslab[done + k, j] if k < DEPTH - 1 else fresh_q
                mixed = mixed - coef_v[done, k][None] * rows_of(r + mixing_weight * q)
            mixed = mixed.reshape(NG, NG)
            if last:
                den_s[pl.ds(2 * j, 2)] = mixed.reshape(2, KEPT, NG).astype(BF16)
            else:
                rslab[DEPTH - 1 + done, j] = fresh_r
                qslab[DEPTH - 1 + done, j] = fresh_q
                pden_v[j] = inside
                pres_v[j] = here
                den_v[j] = mixed
            return carry

        lax.fori_loop(0, 8, one_plane, 0)
        if last:
            leave = pltpu.make_async_copy(den_s, out_d, fin_sems.at[0])
            leave.start()
            leave.wait()
            keep.wait()

    gram = None
    for step in range(ITERS):
        if step == 0:
            for load in loads:
                load.wait()
            facg[...] = jnp.exp(-time_step * (ext_v[...] + den_v[...] - energy_shift))

            def forward(n, carry):
                w = []
                for c in range(2 * PER):
                    at = n * 2 * PER + c
                    f = facg[at % 8]
                    w.append(jnp.concatenate(
                        [bands_v[p, at // 8, at % 8].astype(F32) * f for p in range(2)], axis=1
                    ).astype(BF16))
                for c, b in enumerate(forward_zy(jnp.concatenate(w, axis=0))):
                    send_f[pl.ds((n * 2 * PER + c) * 8, 8)] = b
                return carry

            lax.fori_loop(0, 8 // PER, forward, 0)
            pl.semaphore_wait(barrier, 150)
            columns = [col_of(n) for n in range(8)]

            def first_sends(n, carry):
                which, j = n // 8, n % 8
                for k, q in enumerate(columns):
                    send_tile(
                        send_f.at[n * 8 + q], recv_f.at[8 * i + j], sf_sem, rf_sem, g, 2 * q + which,
                        which == core if k == 7 else None,
                    )
                return carry

            lax.fori_loop(0, 16, first_sends, 0)
            for copy in late:
                copy.start()


            @pl.when(owner)
            def _():
                pieces = [
                    (ext.at[zz], plane.at[0], 0), (den.at[zz], plane.at[1], 0),
                    (pden.at[zz], plane.at[2], 0), (pres.at[zz], plane.at[3], 0),
                    (hden.at[:, zz], rs.at[pl.ds(0, DEPTH - 1)], 1),
                    (hres.at[:, zz], qs.at[pl.ds(0, DEPTH - 1)], 2),
                ]
                for src, dst, s in pieces:
                    pltpu.make_async_copy(src, dst, pl_sems.at[s]).start()
                    remote(src, dst, pl_send.at[s], pl_sems.at[s], g, twin).start()

            occ_row = jnp.full((1, NG), occ[core], F32)
            occ_s[...] = occ_row
            occs[g] = occ_row

            def send_occ(n, c):
                remote(occ_s, occs.at[g], so_sem, ro_sem, (g + n) % 16, i).start()
                return c

            lax.fori_loop(1, 16, send_occ, 0)

        else:
            def forward(n, carry):
                ts = bands_of(n)
                f = facp[...]
                f = jnp.concatenate([f, f], axis=1)
                w = jnp.concatenate([(psi[t].astype(F32) * f).astype(BF16) for t in ts], axis=0)
                for t, b in zip(ts, forward_zy(w)):
                    send_f[pl.ds(t * 8, 8)] = b
                return carry

            lax.fori_loop(0, 8 // PER, forward, 0)
            everyone(lambda dg, q, same: send_tile(
                send_f.at[dg * 8 + q], recv_f.at[me], sf_sem, rf_sem, dg, 2 * q + core, same,
            ))

        if step:
            if step == 1:
                for copy in late:
                    copy.wait()
            slab_update(step - 1)
        spectral()
        drain(send_f.at[pl.ds(0, 120 if step == 0 else 127)], sf_sem)

        if step == 0:
            drain(plane, pl_sems.at[0])
            drain(rs.at[pl.ds(0, DEPTH - 1)], pl_sems.at[1])
            drain(qs.at[pl.ds(0, DEPTH - 1)], pl_sems.at[2])
            drain(occs.at[pl.ds(0, 15)], ro_sem)
            drain(occs.at[pl.ds(0, 15)], so_sem)

            @pl.when(owner)
            def _():
                drain(plane, pl_send.at[0])
                drain(rs.at[pl.ds(0, DEPTH - 1)], pl_send.at[1])
                drain(qs.at[pl.ds(0, DEPTH - 1)], pl_send.at[2])

        part[...] = jnp.zeros_like(part)
        lax.fori_loop(0, 8 // PER, backward, 0)

        swap = remote(part, recv_d.at[step], sd_sem, rd_sems.at[step], g, twin)
        swap.start()
        swap.wait_recv()
        rho_out = (part[...] + recv_d[step]) * (density_scale / bands_total)
        rho_in = plane[1]
        res = rho_out - rho_in
        newest = res - plane[3]
        rs[DEPTH - 1 + step] = rho_in - plane[2]
        qs[DEPTH - 1 + step] = newest

        lanes = lax.broadcasted_iota(jnp.int32, (1, NG), 1)
        row = jnp.zeros((1, NG), F32)

        def put(row, at, a, b):
            total = jnp.sum(jnp.sum(rows_of(a * b), axis=0), axis=0, keepdims=True)
            return jnp.where(lanes == at, jnp.sum(total, axis=1, keepdims=True), row)

        for j in range(DEPTH):
            q = qs[step + j]
            row = put(row, j, q, newest)
            row = put(row, DEPTH + j, q, res)
        if step == 0:
            at = 2 * DEPTH
            for a in range(DEPTH - 1):
                for b in range(a + 1):
                    row = put(row, at, qs[a], qs[b])
                    at += 1
        row_s[...] = row
        rows[me] = row

        def send_row(dg, q, same):
            copy = remote(row_s, rows.at[me], sr_sem, rr_sem, dg, 2 * q + core)
            if same is None:
                copy.start()
            else:
                pl.when(jnp.logical_not(same))(copy.start)

        everyone(send_row)

        outs_s[step] = res.astype(BF16)

        def send_res(m, carry):
            z = z_of(m)
            for h in range(2):
                send_tile(
                    outs_s.at[step, pl.ds(pl.multiple_of(core * KEPT, KEPT), KEPT)],
                    res_v.at[step, 2 * zz + core], sout_sems.at[step], rout_sems.at[step],
                    halves[h] * 8 + z, 2 * xy + half,
                    jnp.logical_and(m == 7, owner) if h == 1 else None,
                )
            return carry

        lax.fori_loop(0, 8, send_res, 0)

        swap.wait_send()
        drain(rows.at[pl.ds(0, 127)], rr_sem)
        drain(rows.at[pl.ds(0, 127)], sr_sem)
        drain(send_b.at[pl.ds(0, 127)], sb_sem)
        sums = jnp.sum(rows[...], axis=0) * (1.0 / (NG * NG * NG))

        def splat(at):
            return jnp.broadcast_to(sums[:, at : at + 1], (8, NG))

        border = [splat(j) for j in range(DEPTH)]
        right = [splat(DEPTH + j) for j in range(DEPTH)]
        if step == 0:
            at = 2 * DEPTH
            gram = []
            for a in range(DEPTH - 1):
                gram.append([splat(at + b) for b in range(a + 1)])
                at += a + 1
        else:
            gram = [[gram[a][b] for b in range(1, a + 1)] for a in range(1, DEPTH)]
        gram.append(border)
        trace = gram[0][0]
        for j in range(1, DEPTH):
            trace = trace + gram[j][j]
        ridge = trace * (ridge_share / DEPTH) + ridge_floor
        low = [[None] * DEPTH for _ in range(DEPTH)]
        scaled = [[None] * DEPTH for _ in range(DEPTH)]
        inverse = [None] * DEPTH
        for c in range(DEPTH):
            value = gram[c][c] + ridge
            for k in range(c):
                value = value - scaled[c][k] * low[c][k]
            inverse[c] = 1.0 / value
            for r in range(c + 1, DEPTH):
                value = gram[r][c]
                for k in range(c):
                    value = value - scaled[r][k] * low[c][k]
                scaled[r][c] = value
                low[r][c] = value * inverse[c]
        middle = []
        for r in range(DEPTH):
            value = right[r]
            for k in range(r):
                value = value - low[r][k] * middle[k]
            middle.append(value)
        coeffs = [None] * DEPTH
        for r in reversed(range(DEPTH)):
            value = middle[r] * inverse[r]
            for k in range(r + 1, DEPTH):
                value = value - low[k][r] * coeffs[k]
            coeffs[r] = value
        for k in range(DEPTH):
            coef_v[step, k] = coeffs[k]
        if step == ITERS - 1:
            break
        mixed = rows_of(rho_in + mixing_weight * res)
        for j in range(DEPTH):
            mixed = mixed - coeffs[j][None] * rows_of(rs[step + j] + mixing_weight * qs[step + j])
        rho = mixed.reshape(NG, NG)
        plane[2] = rho_in
        plane[3] = res
        plane[1] = rho
        facp[...] = jnp.exp(-time_step * (plane[0] + rho - energy_shift))

    slab_update(ITERS - 1)
    for step in range(ITERS):
        @pl.when(owner)
        def _():
            drain(res_v.at[step, pl.ds(0, 15)], sout_sems.at[step])

        @pl.when(jnp.logical_not(owner))
        def _():
            drain(res_v.at[step], sout_sems.at[step])


def local(bands, occupations, external, density_in, prev_density, prev_residual, hist_density, hist_residual):
    slab = external.shape
    hbm = pl.BlockSpec(memory_space=pltpu.HBM)
    smem = pl.BlockSpec(memory_space=pltpu.SMEM)
    dma = pltpu.SemaphoreType.DMA
    both = pl.pallas_call(
        kernel,
        out_shape=[jax.ShapeDtypeStruct((16, KEPT, NG), BF16)] * 2,
        in_specs=[smem] + [hbm] * 8,
        out_specs=[hbm] * 2,
        scratch_shapes=[
            pltpu.VMEM((6 * NG, NG), BF16),
            pltpu.VMEM(bands.shape, BF16),
            pltpu.VMEM(slab, F32),
            pltpu.VMEM(slab, F32),
            pltpu.VMEM(slab, F32),
            pltpu.VMEM((NG, NG), F32),
            pltpu.VMEM((4, NG, NG), F32),
            pltpu.VMEM((DEPTH - 1 + ITERS, NG, NG), F32),
            pltpu.VMEM((DEPTH - 1 + ITERS, NG, NG), F32),
            pltpu.VMEM((16, NG, 2 * NG), BF16),
            pltpu.VMEM((128, 8, NG), BF16),
            pltpu.VMEM((128, 8, NG), BF16),
            pltpu.VMEM((8 * NG, NG), F32),
            pltpu.VMEM((8, KEPT, NG), F32),
            pltpu.VMEM((128, 8, NG), BF16),
            pltpu.VMEM((128, 8, NG), BF16),
            pltpu.VMEM((NG, NG), F32),
            pltpu.VMEM((ITERS, NG, NG), F32),
            pltpu.VMEM((1, NG), F32),
            pltpu.VMEM((128, 1, NG), F32),
            pltpu.VMEM((1, NG), F32),
            pltpu.VMEM((16, 1, NG), F32),
            pltpu.VMEM((ITERS, NG, NG), BF16),
            pltpu.VMEM((ITERS, 16, KEPT, NG), BF16),
            pltpu.VMEM((16, KEPT, NG), BF16),
            pltpu.VMEM((DEPTH - 1 + ITERS, *slab), F32),
            pltpu.VMEM((DEPTH - 1 + ITERS, *slab), F32),
            pltpu.VMEM(slab, F32),
            pltpu.VMEM(slab, F32),
            pltpu.VMEM((ITERS, DEPTH, 8, NG), F32),
            dma((4,)), dma((3,)), dma((3,)),
            dma(()), dma(()), dma(()), dma((16,)), dma(()), dma((ITERS,)),
            dma(()), dma(()), dma(()), dma(()), dma((ITERS,)), dma((ITERS,)), dma((4,)), dma((2,)),
        ],
        compiler_params=pltpu.CompilerParams(
            has_side_effects=True, collective_id=0, vmem_limit_bytes=67043328
        ),
        name="scf",
    )(
        occupations, bands, external, density_in, prev_density, prev_residual,
        hist_density, hist_residual, jnp.asarray(tables()),
    )
    return tuple(half.reshape(slab).astype(F32) for half in both)


def solution(mesh):
    placed = (
        P(None, "band", "grid", None, None),
        P("band"),
        P("grid", None, None),
        P("grid", None, None),
        P("grid", None, None),
        P("grid", None, None),
        P(None, "grid", None, None),
        P(None, "grid", None, None),
    )
    return jax.shard_map(
        local,
        mesh=mesh,
        in_specs=placed,
        out_specs=(P("grid", None, None), P("grid", None, None)),
        check_vma=False,
    )
```

```python
import math

import jax
import jax.numpy as jnp
import ml_dtypes
import numpy as np
from jax import lax
from jax.experimental import pallas as pl
from jax.experimental.pallas import tpu as pltpu
from jax.sharding import PartitionSpec as P

NG = 128
KEPT = NG // 2
DEPTH = 6
ITERS = 3
PF = 4
PB = 4
F32 = jnp.float32
BF16 = jnp.bfloat16
MESH = pl.DeviceIdType.MESH

time_step = 0.25
energy_shift = 2.5
mixing_weight = 0.5
ridge_share = 0.1
ridge_floor = 0.01
density_scale = 8.0
bands_total = 32


def tables():
    frequency = np.arange(-(NG // 4), NG // 4, dtype=np.int32)
    positions = np.arange(NG, dtype=np.int32)
    phase = (positions[:, None] * frequency[None, :]) % NG
    angles = phase.astype(np.float32) * np.float32(2.0 * math.pi / NG)
    unit = np.float32(1.0 / math.sqrt(NG))
    cosine = (np.cos(angles) * unit).astype(ml_dtypes.bfloat16)
    sine = (np.sin(angles) * unit).astype(ml_dtypes.bfloat16)
    forward_z = np.concatenate(
        [np.concatenate([cosine, -sine], 1), np.concatenate([sine, cosine], 1)], 0
    )
    inverse_z = np.concatenate(
        [np.concatenate([cosine.T, sine.T], 1), np.concatenate([-sine.T, cosine.T], 1)], 0
    )
    stacked = np.concatenate([cosine.T, sine.T], 0)
    beside = np.concatenate([cosine, sine], 1)
    return np.concatenate(
        [forward_z, stacked, beside, inverse_z[:, :NG], inverse_z[:, NG:]], 0
    )


def dot(a, b):
    return jnp.dot(a, b, preferred_element_type=F32)


def kernel(
    occ, bands, ext, den, pden, pres, hden, hres, mats,
    out_d, out_r,
    mats_v, bands_v, ext_v, den_v, facg, facp, plane, rs, qs, psi,
    send_f, recv_f, stage, kin, send_b, recv_b, part, recv_d, row_s, rows, occ_s, occs,
    outs_s, res_v, den_s, rslab, qslab, pden_v, pres_v, coef_v,
    in_sems, pl_sems, pl_send, sf_sem, rf_sem, sb_sem, rb_sems, sd_sem, rd_sems,
    sr_sem, rr_sem, so_sem, ro_sem, sout_sems, rout_sems, late_sems, fin_sems,
):
    g = lax.axis_index("band")
    i = lax.axis_index("grid")
    core = i % 2
    xy = i // 2
    half = g // 8
    zz = g % 8
    me = xy * 16 + g
    twin = i + 1 - 2 * core
    owner = core == half

    def remote(src, dst, ssem, rsem, dg, di):
        return pltpu.make_async_remote_copy(
            src_ref=src, dst_ref=dst, send_sem=ssem, recv_sem=rsem,
            device_id=(dg, di), device_id_type=MESH,
        )

    def drain(ref, sem):
        pltpu.make_async_copy(ref, ref, sem).wait()

    loads = [
        pltpu.make_async_copy(ext, ext_v, in_sems.at[0]),
        pltpu.make_async_copy(den, den_v, in_sems.at[1]),
        pltpu.make_async_copy(bands, bands_v, in_sems.at[2]),
        pltpu.make_async_copy(mats, mats_v, in_sems.at[3]),
    ]
    for load in loads:
        load.start()
    late = [
        pltpu.make_async_copy(hden, rslab.at[pl.ds(0, DEPTH - 1)], late_sems.at[0]),
        pltpu.make_async_copy(hres, qslab.at[pl.ds(0, DEPTH - 1)], late_sems.at[1]),
        pltpu.make_async_copy(pden, pden_v, late_sems.at[2]),
        pltpu.make_async_copy(pres, pres_v, late_sems.at[3]),
    ]

    def z_of(m):
        return (zz + 4 + (1 - 2 * (m % 2)) * ((m + 1) // 2)) % 8

    def col_of(n):
        k = n // 2
        dx = 2 + (1 - 2 * (k % 2)) * ((k + 1) // 2)
        return ((xy // 2 + dx) % 4) * 2 + (xy + 1 - n % 2) % 2

    halves = [1 - half, half]
    rings = [halves[h] * 8 + z_of(m) for m in range(8) for h in range(2)]

    def everyone(start):
        def column(n, carry):
            q = col_of(n)
            for at, dg in enumerate(rings):
                start(dg, q, n == 7 if at == 15 else None)
            return carry

        lax.fori_loop(0, 8, column, 0)

    columns = [col_of(n) for n in range(8)]

    def hops(n, at):
        dx, dz = (2, 1, 1, 0)[n // 2], (4, 3, 3, 2, 2, 1, 1, 0)[at // 2]
        return dx + dz + (2 * (1 - n % 2) if at % 2 else 1)

    far_first = sorted(
        [(n, at) for n in range(8) for at in range(16) if (n, at) != (7, 15)],
        key=lambda p: -hops(*p),
    )


    barrier = pltpu.get_barrier_semaphore()

    def hello(dg, di):
        pl.semaphore_signal(barrier, inc=1, device_id=(dg, di), device_id_type=MESH)

    def greet(dg, q, same):
        if same is None:
            hello(dg, 2 * q + core)
        else:
            pl.when(jnp.logical_not(same))(lambda: hello(dg, 2 * q + core))

    everyone(greet)
    for dg in rings:
        hello(dg, twin)

    def greet_column(n, carry):
        hello(g, 2 * col_of(n) + 1 - core)
        return carry

    lax.fori_loop(0, 7, greet_column, 0)

    lane = lax.broadcasted_iota(jnp.int32, (KEPT, NG), 1)
    sgn_f = jnp.where(lane < KEPT, 1.0, -1.0).astype(F32)
    sgn_i = -sgn_f
    fz = (lane % KEPT - NG // 4).astype(F32)
    fx = (lax.broadcasted_iota(jnp.int32, (KEPT, NG), 0) - NG // 4).astype(F32)
    quarter = NG / 4.0
    for r in range(8):
        fy = (8 * xy + r - NG // 4).astype(F32)
        kin[r] = jnp.exp((fx * fx + fy * fy + fz * fz) * (-time_step / (quarter * quarter)))

    wzf, fcs, ics = mats_v.at[pl.ds(0, 2 * NG)], mats_v.at[pl.ds(2 * NG, NG)], mats_v.at[pl.ds(3 * NG, NG)]
    wzi = mats_v.at[pl.ds(4 * NG, NG)], mats_v.at[pl.ds(5 * NG, NG)]

    def turned(a):
        return pltpu.roll(a, KEPT, 1)

    def pair_forward(x):
        pq = dot(fcs[...], x)
        return [
            pq[:KEPT, c : c + NG] + turned(pq[KEPT:, c : c + NG]) * sgn_f for c in (0, NG)
        ]

    def pair_inverse(d):
        both = [jnp.concatenate([v, turned(v) * sgn_i], axis=0).astype(BF16) for v in d]
        return dot(ics[...], jnp.concatenate(both, axis=1))

    def forward_zy(w):
        a = dot(w, wzf[...]).astype(BF16)
        out = []
        for at in range(0, w.shape[0], 2 * NG):
            b = pair_forward(jnp.concatenate([a[at : at + NG], a[at + NG : at + 2 * NG]], axis=1))
            out += [v.reshape(8, 8, NG).astype(BF16) for v in b]
        return out

    def send_tile(src, dst, ssem, rsem, dg, di, same=None):
        if same is None:
            remote(src, dst, ssem, rsem, dg, di).start()
            return

        @pl.when(same)
        def _():
            pltpu.make_async_copy(src, dst, rsem).start()

        @pl.when(jnp.logical_not(same))
        def _():
            remote(src, dst, ssem, rsem, dg, di).start()

    def spectral():
        drain(recv_f, rf_sem)
        stage[...] = recv_f[...].astype(F32).reshape(8 * NG, NG)
        for r in range(0, 8, 2):
            x = [stage[pl.ds(r + c, NG, stride=8), :].astype(BF16) for c in range(2)]
            b = pair_forward(jnp.concatenate(x, axis=1))
            y = pair_inverse([b[c] * kin[r + c] for c in range(2)])
            for c in range(2):
                stage[pl.ds(r + c, NG, stride=8), :] = y[:, c * NG : (c + 1) * NG]
        send_b[...] = stage[...].reshape(NG, 8, NG).astype(BF16)

        pltpu.make_async_copy(send_b.at[me], recv_b.at[g * 8 + xy], rb_sems.at[g]).start()
        for n, at in far_first:
            q, dg = columns[n], rings[at]
            send_tile(
                send_b.at[q * 16 + dg], recv_b.at[g * 8 + xy], sb_sem, rb_sems.at[g],
                dg, 2 * q + core,
            )

    def bands_of(n, per):
        return [halves[h] * 8 + z_of(n * per + e) for e in range(per) for h in range(2)]

    def backward(n, carry):
        ts = bands_of(n, PB)
        d = []
        for t in ts:
            tiles = recv_b.at[pl.ds(t * 8, 8)]
            drain(tiles, rb_sems.at[t])
            d.append(tiles[...].astype(F32).reshape(KEPT, NG))
        e = []
        for at in range(0, len(ts), 2):
            both = pair_inverse(d[at : at + 2])
            e += [both[:, :NG], both[:, NG:]]
        e = jnp.concatenate(e, axis=0).astype(BF16)
        re = dot(e, wzi[0][...]).astype(BF16)
        im = dot(e, wzi[1][...]).astype(BF16)
        total = part[...]
        for h, t in enumerate(ts):
            mine = slice(h * NG, (h + 1) * NG)
            psi[t, :, :NG] = re[mine]
            psi[t, :, NG:] = im[mine]
            wide_re, wide_im = re[mine].astype(F32), im[mine].astype(F32)
            total = total + occs[t] * (wide_re * wide_re + wide_im * wide_im)
        part[...] = total
        return carry

    def rows_of(a):
        return a.reshape(16, 8, NG)

    def slab_update(done):
        drain(res_v.at[done], rout_sems.at[done])
        last = done == ITERS - 1
        if last:
            keep = pltpu.make_async_copy(res_v.at[done], out_r, fin_sems.at[1])
            keep.start()

        def one_plane(j, carry):
            here = res_v[done, pl.ds(2 * j, 2)].astype(F32).reshape(NG, NG)
            inside = den_v[j]
            fresh_r, fresh_q = inside - pden_v[j], here - pres_v[j]
            mixed = rows_of(inside + mixing_weight * here)
            for k in range(DEPTH):
                if k == DEPTH - 1:
                    move = fresh_r + mixing_weight * fresh_q
                elif last:
                    move = rslab[done + k, j]
                else:
                    move = rslab[done + k, j] + mixing_weight * qslab[done + k, j]
                mixed = mixed - coef_v[done, k][None] * rows_of(move)
            mixed = mixed.reshape(NG, NG)
            if last:
                den_s[pl.ds(2 * j, 2)] = mixed.reshape(2, KEPT, NG).astype(BF16)
                pltpu.make_async_copy(
                    den_s.at[pl.ds(2 * j, 2)], out_d.at[pl.ds(2 * j, 2)], fin_sems.at[0]
                ).start()
            else:
                rslab[DEPTH - 1 + done, j] = fresh_r
                qslab[DEPTH - 1 + done, j] = fresh_q
                pden_v[j] = inside
                pres_v[j] = here
                den_v[j] = mixed
            return carry

        lax.fori_loop(0, 8, one_plane, 0)
        if last:
            pltpu.make_async_copy(den_s, out_d, fin_sems.at[0]).wait()
            keep.wait()

    gram = None
    for step in range(ITERS):
        if step == 0:
            for load in loads:
                load.wait()
            facg[...] = jnp.exp(-time_step * (ext_v[...] + den_v[...] - energy_shift))

            def forward(n, carry):
                w = []
                for c in range(2 * PF):
                    at = n * 2 * PF + c
                    f = facg[at % 8]
                    w.append(jnp.concatenate(
                        [bands_v[p, at // 8, at % 8].astype(F32) * f for p in range(2)], axis=1
                    ).astype(BF16))
                for c, b in enumerate(forward_zy(jnp.concatenate(w, axis=0))):
                    send_f[pl.ds((n * 2 * PF + c) * 8, 8)] = b
                return carry

            lax.fori_loop(0, 8 // PF, forward, 0)
            pl.semaphore_wait(barrier, 150)

            def first_sends(n, carry):
                which, j = n // 8, n % 8
                for k, q in enumerate(columns):
                    send_tile(
                        send_f.at[n * 8 + q], recv_f.at[8 * i + j], sf_sem, rf_sem, g, 2 * q + which,
                        which == core if k == 7 else None,
                    )
                return carry

            lax.fori_loop(0, 16, first_sends, 0)
            for copy in late:
                copy.start()


            @pl.when(owner)
            def _():
                pieces = [
                    (ext.at[zz], plane.at[0], 0), (den.at[zz], plane.at[1], 0),
                    (pden.at[zz], plane.at[2], 0), (pres.at[zz], plane.at[3], 0),
                    (hden.at[:, zz], rs.at[pl.ds(0, DEPTH - 1)], 1),
                    (hres.at[:, zz], qs.at[pl.ds(0, DEPTH - 1)], 2),
                ]
                for src, dst, s in pieces:
                    pltpu.make_async_copy(src, dst, pl_sems.at[s]).start()
                    remote(src, dst, pl_send.at[s], pl_sems.at[s], g, twin).start()

            occ_row = jnp.full((1, NG), occ[core], F32)
            occ_s[...] = occ_row
            occs[g] = occ_row

            def send_occ(n, c):
                remote(occ_s, occs.at[g], so_sem, ro_sem, (g + n) % 16, i).start()
                return c

            lax.fori_loop(1, 16, send_occ, 0)

        else:
            def forward(n, carry):
                ts = bands_of(n, PF)
                f = facp[...]
                f = jnp.concatenate([f, f], axis=1)
                w = jnp.concatenate([(psi[t].astype(F32) * f).astype(BF16) for t in ts], axis=0)
                for t, b in zip(ts, forward_zy(w)):
                    send_f[pl.ds(t * 8, 8)] = b
                return carry

            lax.fori_loop(0, 8 // PF, forward, 0)
            pltpu.make_async_copy(send_f.at[g * 8 + xy], recv_f.at[me], rf_sem).start()
            for n, at in far_first:
                q, dg = columns[n], rings[at]
                send_tile(
                    send_f.at[dg * 8 + q], recv_f.at[me], sf_sem, rf_sem, dg, 2 * q + core
                )

        if step:
            if step == 1:
                for copy in late:
                    copy.wait()
            slab_update(step - 1)
        spectral()
        drain(send_f.at[pl.ds(0, 120 if step == 0 else 127)], sf_sem)

        if step == 0:
            drain(plane, pl_sems.at[0])
            drain(rs.at[pl.ds(0, DEPTH - 1)], pl_sems.at[1])
            drain(qs.at[pl.ds(0, DEPTH - 1)], pl_sems.at[2])
            drain(occs.at[pl.ds(0, 15)], ro_sem)
            drain(occs.at[pl.ds(0, 15)], so_sem)

            @pl.when(owner)
            def _():
                drain(plane, pl_send.at[0])
                drain(rs.at[pl.ds(0, DEPTH - 1)], pl_send.at[1])
                drain(qs.at[pl.ds(0, DEPTH - 1)], pl_send.at[2])

        part[...] = jnp.zeros_like(part)
        lax.fori_loop(0, 8 // PB, backward, 0)

        swap = remote(part, recv_d.at[step], sd_sem, rd_sems.at[step], g, twin)
        swap.start()
        swap.wait_recv()
        rho_out = (part[...] + recv_d[step]) * (density_scale / bands_total)
        rho_in = plane[1]
        res = rho_out - rho_in
        newest = res - plane[3]
        rs[DEPTH - 1 + step] = rho_in - plane[2]
        qs[DEPTH - 1 + step] = newest

        lanes = lax.broadcasted_iota(jnp.int32, (1, NG), 1)
        row = jnp.zeros((1, NG), F32)

        def put(row, at, a, b):
            total = jnp.sum(jnp.sum(rows_of(a * b), axis=0), axis=0, keepdims=True)
            return jnp.where(lanes == at, jnp.sum(total, axis=1, keepdims=True), row)

        for j in range(DEPTH):
            q = qs[step + j]
            row = put(row, j, q, newest)
            row = put(row, DEPTH + j, q, res)
        if step == 0:
            at = 2 * DEPTH
            for a in range(DEPTH - 1):
                for b in range(a + 1):
                    row = put(row, at, qs[a], qs[b])
                    at += 1
        row_s[...] = row
        rows[me] = row

        for n, at in far_first:
            remote(
                row_s, rows.at[me], sr_sem, rr_sem, rings[at], 2 * columns[n] + core
            ).start()

        outs_s[step] = res.astype(BF16)

        def send_res(m, carry):
            z = z_of(m)
            for h in range(2):
                send_tile(
                    outs_s.at[step, pl.ds(pl.multiple_of(core * KEPT, KEPT), KEPT)],
                    res_v.at[step, 2 * zz + core], sout_sems.at[step], rout_sems.at[step],
                    halves[h] * 8 + z, 2 * xy + half,
                    jnp.logical_and(m == 7, owner) if h == 1 else None,
                )
            return carry

        lax.fori_loop(0, 8, send_res, 0)

        if step == ITERS - 1:
            def join(j, carry):
                for k in range(step, step + DEPTH - 1):
                    rslab[k, j] = rslab[k, j] + mixing_weight * qslab[k, j]
                return carry

            lax.fori_loop(0, 8, join, 0)

        swap.wait_send()
        drain(rows.at[pl.ds(0, 127)], rr_sem)
        drain(rows.at[pl.ds(0, 127)], sr_sem)
        drain(send_b.at[pl.ds(0, 127)], sb_sem)
        sums = jnp.sum(rows[...], axis=0) * (1.0 / (NG * NG * NG))

        def splat(at):
            return jnp.broadcast_to(sums[:, at : at + 1], (8, NG))

        border = [splat(j) for j in range(DEPTH)]
        right = [splat(DEPTH + j) for j in range(DEPTH)]
        if step == 0:
            at = 2 * DEPTH
            gram = []
            for a in range(DEPTH - 1):
                gram.append([splat(at + b) for b in range(a + 1)])
                at += a + 1
        else:
            gram = [[gram[a][b] for b in range(1, a + 1)] for a in range(1, DEPTH)]
        gram.append(border)
        trace = gram[0][0]
        for j in range(1, DEPTH):
            trace = trace + gram[j][j]
        ridge = trace * (ridge_share / DEPTH) + ridge_floor
        low = [[None] * DEPTH for _ in range(DEPTH)]
        scaled = [[None] * DEPTH for _ in range(DEPTH)]
        inverse = [None] * DEPTH
        for c in range(DEPTH):
            value = gram[c][c] + ridge
            for k in range(c):
                value = value - scaled[c][k] * low[c][k]
            inverse[c] = 1.0 / value
            for r in range(c + 1, DEPTH):
                value = gram[r][c]
                for k in range(c):
                    value = value - scaled[r][k] * low[c][k]
                scaled[r][c] = value
                low[r][c] = value * inverse[c]
        middle = []
        for r in range(DEPTH):
            value = right[r]
            for k in range(r):
                value = value - low[r][k] * middle[k]
            middle.append(value)
        coeffs = [None] * DEPTH
        for r in reversed(range(DEPTH)):
            value = middle[r] * inverse[r]
            for k in range(r + 1, DEPTH):
                value = value - low[k][r] * coeffs[k]
            coeffs[r] = value
        for k in range(DEPTH):
            coef_v[step, k] = coeffs[k]
        if step == ITERS - 1:
            break
        mixed = rows_of(rho_in + mixing_weight * res)
        for j in range(DEPTH):
            mixed = mixed - coeffs[j][None] * rows_of(rs[step + j] + mixing_weight * qs[step + j])
        rho = mixed.reshape(NG, NG)
        plane[2] = rho_in
        plane[3] = res
        plane[1] = rho
        facp[...] = jnp.exp(-time_step * (plane[0] + rho - energy_shift))

    slab_update(ITERS - 1)
    for step in range(ITERS):
        @pl.when(owner)
        def _():
            drain(res_v.at[step, pl.ds(0, 15)], sout_sems.at[step])

        @pl.when(jnp.logical_not(owner))
        def _():
            drain(res_v.at[step], sout_sems.at[step])


def local(bands, occupations, external, density_in, prev_density, prev_residual, hist_density, hist_residual):
    slab = external.shape
    hbm = pl.BlockSpec(memory_space=pltpu.HBM)
    smem = pl.BlockSpec(memory_space=pltpu.SMEM)
    dma = pltpu.SemaphoreType.DMA
    both = pl.pallas_call(
        kernel,
        out_shape=[jax.ShapeDtypeStruct((16, KEPT, NG), BF16)] * 2,
        in_specs=[smem] + [hbm] * 8,
        out_specs=[hbm] * 2,
        scratch_shapes=[
            pltpu.VMEM((6 * NG, NG), BF16),
            pltpu.VMEM(bands.shape, BF16),
            pltpu.VMEM(slab, F32),
            pltpu.VMEM(slab, F32),
            pltpu.VMEM(slab, F32),
            pltpu.VMEM((NG, NG), F32),
            pltpu.VMEM((4, NG, NG), F32),
            pltpu.VMEM((DEPTH - 1 + ITERS, NG, NG), F32),
            pltpu.VMEM((DEPTH - 1 + ITERS, NG, NG), F32),
            pltpu.VMEM((16, NG, 2 * NG), BF16),
            pltpu.VMEM((128, 8, NG), BF16),
            pltpu.VMEM((128, 8, NG), BF16),
            pltpu.VMEM((8 * NG, NG), F32),
            pltpu.VMEM((8, KEPT, NG), F32),
            pltpu.VMEM((128, 8, NG), BF16),
            pltpu.VMEM((128, 8, NG), BF16),
            pltpu.VMEM((NG, NG), F32),
            pltpu.VMEM((ITERS, NG, NG), F32),
            pltpu.VMEM((1, NG), F32),
            pltpu.VMEM((128, 1, NG), F32),
            pltpu.VMEM((1, NG), F32),
            pltpu.VMEM((16, 1, NG), F32),
            pltpu.VMEM((ITERS, NG, NG), BF16),
            pltpu.VMEM((ITERS, 16, KEPT, NG), BF16),
            pltpu.VMEM((16, KEPT, NG), BF16),
            pltpu.VMEM((DEPTH - 1 + ITERS, *slab), F32),
            pltpu.VMEM((DEPTH - 1 + ITERS, *slab), F32),
            pltpu.VMEM(slab, F32),
            pltpu.VMEM(slab, F32),
            pltpu.VMEM((ITERS, DEPTH, 8, NG), F32),
            dma((4,)), dma((3,)), dma((3,)),
            dma(()), dma(()), dma(()), dma((16,)), dma(()), dma((ITERS,)),
            dma(()), dma(()), dma(()), dma(()), dma((ITERS,)), dma((ITERS,)), dma((4,)), dma((2,)),
        ],
        compiler_params=pltpu.CompilerParams(
            has_side_effects=True, collective_id=0, vmem_limit_bytes=67043328
        ),
        name="scf",
    )(
        occupations, bands, external, density_in, prev_density, prev_residual,
        hist_density, hist_residual, jnp.asarray(tables()),
    )
    return tuple(half.reshape(slab).astype(F32) for half in both)


def solution(mesh):
    placed = (
        P(None, "band", "grid", None, None),
        P("band"),
        P("grid", None, None),
        P("grid", None, None),
        P("grid", None, None),
        P("grid", None, None),
        P(None, "grid", None, None),
        P(None, "grid", None, None),
    )
    return jax.shard_map(
        local,
        mesh=mesh,
        in_specs=placed,
        out_specs=(P("grid", None, None), P("grid", None, None)),
        check_vma=False,
    )
```

```python
import functools
import math

import jax
import jax.numpy as jnp
import ml_dtypes
import numpy as np
from jax import lax
from jax.experimental import pallas as pl
from jax.experimental.pallas import tpu as pltpu
from jax.sharding import PartitionSpec as P

NG = 128
KEPT = NG // 2
DEPTH = 6
ITERS = 3
PF = 4
PB = 4
F32 = jnp.float32
BF16 = jnp.bfloat16
MESH = pl.DeviceIdType.MESH

time_step = 0.25
energy_shift = 2.5
mixing_weight = 0.5
ridge_share = 0.1
ridge_floor = 0.01
density_scale = 8.0
bands_total = 32


def tables():
    frequency = np.arange(-(NG // 4), NG // 4, dtype=np.int32)
    positions = np.arange(NG, dtype=np.int32)
    phase = (positions[:, None] * frequency[None, :]) % NG
    angles = phase.astype(np.float32) * np.float32(2.0 * math.pi / NG)
    unit = np.float32(1.0 / math.sqrt(NG))
    cosine = (np.cos(angles) * unit).astype(ml_dtypes.bfloat16)
    sine = (np.sin(angles) * unit).astype(ml_dtypes.bfloat16)
    forward_z = np.concatenate(
        [np.concatenate([cosine, -sine], 1), np.concatenate([sine, cosine], 1)], 0
    )
    inverse_z = np.concatenate(
        [np.concatenate([cosine.T, sine.T], 1), np.concatenate([-sine.T, cosine.T], 1)], 0
    )
    stacked = np.concatenate([cosine.T, sine.T], 0)
    beside = np.concatenate([cosine, sine], 1)
    return np.concatenate(
        [forward_z, stacked, beside, inverse_z[:, :NG], inverse_z[:, NG:]], 0
    )


def dot(a, b):
    return jnp.dot(a, b, preferred_element_type=F32)


def kernel(
    occ, bands, ext, den, pden, pres, hden, hres, mats,
    out_d, out_r,
    mats_v, bands_v, ext_v, den_v, facg, facp, plane, rs, qs, psi,
    send_f, recv_f, stage, kin, send_b, recv_b, part, recv_d, row_s, rows, occ_s, occs,
    outs_s, res_v, den_s, rslab, qslab, pden_v, pres_v, coef_v,
    in_sems, pl_sems, pl_send, sf_sem, rf_sem, sb_sem, rb_sems, sd_sem, rd_sems,
    sr_sem, rr_sem, so_sem, ro_sem, sout_sems, rout_sems, late_sems, fin_sems,
):
    g = lax.axis_index("band")
    i = lax.axis_index("grid")
    core = i % 2
    xy = i // 2
    half = g // 8
    zz = g % 8
    me = xy * 16 + g
    twin = i + 1 - 2 * core
    owner = core == half

    def remote(src, dst, ssem, rsem, dg, di):
        return pltpu.make_async_remote_copy(
            src_ref=src, dst_ref=dst, send_sem=ssem, recv_sem=rsem,
            device_id=(dg, di), device_id_type=MESH,
        )

    def drain(ref, sem):
        pltpu.make_async_copy(ref, ref, sem).wait()

    loads = [
        pltpu.make_async_copy(ext, ext_v, in_sems.at[0]),
        pltpu.make_async_copy(den, den_v, in_sems.at[1]),
        pltpu.make_async_copy(bands, bands_v, in_sems.at[2]),
        pltpu.make_async_copy(mats, mats_v, in_sems.at[3]),
    ]
    for load in loads:
        load.start()
    late = [
        pltpu.make_async_copy(hden, rslab.at[pl.ds(0, DEPTH - 1)], late_sems.at[0]),
        pltpu.make_async_copy(hres, qslab.at[pl.ds(0, DEPTH - 1)], late_sems.at[1]),
        pltpu.make_async_copy(pden, pden_v, late_sems.at[2]),
        pltpu.make_async_copy(pres, pres_v, late_sems.at[3]),
    ]

    def z_of(m):
        return (zz + 4 + (1 - 2 * (m % 2)) * ((m + 1) // 2)) % 8

    def col_of(n):
        k = n // 2
        dx = 2 + (1 - 2 * (k % 2)) * ((k + 1) // 2)
        return ((xy // 2 + dx) % 4) * 2 + (xy + 1 - n % 2) % 2

    halves = [1 - half, half]
    rings = [halves[h] * 8 + z_of(m) for m in range(8) for h in range(2)]

    def everyone(start):
        def column(n, carry):
            q = col_of(n)
            for at, dg in enumerate(rings):
                start(dg, q, n == 7 if at == 15 else None)
            return carry

        lax.fori_loop(0, 8, column, 0)

    columns = [col_of(n) for n in range(8)]

    def hops(n, at):
        dx, dz = (2, 1, 1, 0)[n // 2], (4, 3, 3, 2, 2, 1, 1, 0)[at // 2]
        return dx + dz + (2 * (1 - n % 2) if at % 2 else 1)

    far_first = sorted(
        [(n, at) for n in range(8) for at in range(16) if (n, at) != (7, 15)],
        key=lambda p: -hops(*p),
    )


    barrier = pltpu.get_barrier_semaphore()

    def hello(dg, di):
        pl.semaphore_signal(barrier, inc=1, device_id=(dg, di), device_id_type=MESH)

    def greet(dg, q, same):
        if same is None:
            hello(dg, 2 * q + core)
        else:
            pl.when(jnp.logical_not(same))(lambda: hello(dg, 2 * q + core))

    everyone(greet)
    for dg in rings:
        hello(dg, twin)

    def greet_column(n, carry):
        hello(g, 2 * col_of(n) + 1 - core)
        return carry

    lax.fori_loop(0, 7, greet_column, 0)

    lane = lax.broadcasted_iota(jnp.int32, (KEPT, NG), 1)
    sgn_f = jnp.where(lane < KEPT, 1.0, -1.0).astype(F32)
    sgn_i = -sgn_f
    fz = (lane % KEPT - NG // 4).astype(F32)
    fx = (lax.broadcasted_iota(jnp.int32, (KEPT, NG), 0) - NG // 4).astype(F32)
    quarter = NG / 4.0
    for r in range(8):
        fy = (8 * xy + r - NG // 4).astype(F32)
        kin[r] = jnp.exp((fx * fx + fy * fy + fz * fz) * (-time_step / (quarter * quarter)))

    wzf, fcs, ics = mats_v.at[pl.ds(0, 2 * NG)], mats_v.at[pl.ds(2 * NG, NG)], mats_v.at[pl.ds(3 * NG, NG)]
    wzi = mats_v.at[pl.ds(4 * NG, NG)], mats_v.at[pl.ds(5 * NG, NG)]

    def turned(a):
        return pltpu.roll(a, KEPT, 1)

    def pair_forward(x):
        pq = dot(fcs[...], x)
        return [
            pq[:KEPT, c : c + NG] + turned(pq[KEPT:, c : c + NG]) * sgn_f for c in (0, NG)
        ]

    def pair_inverse(d):
        both = [jnp.concatenate([v, turned(v) * sgn_i], axis=0).astype(BF16) for v in d]
        return dot(ics[...], jnp.concatenate(both, axis=1))

    def forward_zy(w):
        a = dot(w, wzf[...]).astype(BF16)
        out = []
        for at in range(0, w.shape[0], 2 * NG):
            b = pair_forward(jnp.concatenate([a[at : at + NG], a[at + NG : at + 2 * NG]], axis=1))
            out += [v.reshape(8, 8, NG).astype(BF16) for v in b]
        return out

    def send_tile(src, dst, ssem, rsem, dg, di, same=None):
        if same is None:
            remote(src, dst, ssem, rsem, dg, di).start()
            return

        @pl.when(same)
        def _():
            pltpu.make_async_copy(src, dst, rsem).start()

        @pl.when(jnp.logical_not(same))
        def _():
            remote(src, dst, ssem, rsem, dg, di).start()

    def spectral():
        drain(recv_f, rf_sem)
        stage[...] = recv_f[...].astype(F32).reshape(8 * NG, NG)
        for r in range(0, 8, 2):
            x = [stage[pl.ds(r + c, NG, stride=8), :].astype(BF16) for c in range(2)]
            b = pair_forward(jnp.concatenate(x, axis=1))
            y = pair_inverse([b[c] * kin[r + c] for c in range(2)])
            for c in range(2):
                stage[pl.ds(r + c, NG, stride=8), :] = y[:, c * NG : (c + 1) * NG]
        send_b[...] = stage[...].reshape(NG, 8, NG).astype(BF16)

        pltpu.make_async_copy(send_b.at[me], recv_b.at[g * 8 + xy], rb_sems.at[g]).start()
        for n, at in far_first:
            q, dg = columns[n], rings[at]
            send_tile(
                send_b.at[q * 16 + dg], recv_b.at[g * 8 + xy], sb_sem, rb_sems.at[g],
                dg, 2 * q + core,
            )

    def bands_of(n, per):
        return [halves[h] * 8 + z_of(n * per + e) for e in range(per) for h in range(2)]

    def backward(n, carry, keep=True):
        ts = bands_of(n, PB)
        d = []
        for t in ts:
            tiles = recv_b.at[pl.ds(t * 8, 8)]
            drain(tiles, rb_sems.at[t])
            d.append(tiles[...].astype(F32).reshape(KEPT, NG))
        e = []
        for at in range(0, len(ts), 2):
            both = pair_inverse(d[at : at + 2])
            e += [both[:, :NG], both[:, NG:]]
        e = jnp.concatenate(e, axis=0).astype(BF16)
        re = dot(e, wzi[0][...]).astype(BF16)
        im = dot(e, wzi[1][...]).astype(BF16)
        total = part[...]
        for h, t in enumerate(ts):
            mine = slice(h * NG, (h + 1) * NG)
            if keep:
                psi[t, :, :NG] = re[mine]
                psi[t, :, NG:] = im[mine]
            wide_re, wide_im = re[mine].astype(F32), im[mine].astype(F32)
            total = total + occs[t] * (wide_re * wide_re + wide_im * wide_im)
        part[...] = total
        return carry

    def rows_of(a):
        return a.reshape(16, 8, NG)

    def slab_update(done):
        drain(res_v.at[done], rout_sems.at[done])
        last = done == ITERS - 1
        if last:
            keep = pltpu.make_async_copy(res_v.at[done], out_r, fin_sems.at[1])
            keep.start()

        def one_plane(j, carry):
            here = res_v[done, pl.ds(2 * j, 2)].astype(F32).reshape(NG, NG)
            inside = den_v[j]
            fresh_r, fresh_q = inside - pden_v[j], here - pres_v[j]
            mixed = rows_of(inside + mixing_weight * here)
            for k in range(DEPTH):
                if k == DEPTH - 1:
                    move = fresh_r + mixing_weight * fresh_q
                elif last:
                    move = rslab[done + k, j]
                else:
                    move = rslab[done + k, j] + mixing_weight * qslab[done + k, j]
                mixed = mixed - coef_v[done, k][None] * rows_of(move)
            mixed = mixed.reshape(NG, NG)
            if last:
                den_s[pl.ds(2 * j, 2)] = mixed.reshape(2, KEPT, NG).astype(BF16)
                pltpu.make_async_copy(
                    den_s.at[pl.ds(2 * j, 2)], out_d.at[pl.ds(2 * j, 2)], fin_sems.at[0]
                ).start()
            else:
                rslab[DEPTH - 1 + done, j] = fresh_r
                qslab[DEPTH - 1 + done, j] = fresh_q
                pden_v[j] = inside
                pres_v[j] = here
                den_v[j] = mixed
            return carry

        lax.fori_loop(0, 8, one_plane, 0)
        if last:
            pltpu.make_async_copy(den_s, out_d, fin_sems.at[0]).wait()
            keep.wait()

    gram = None
    for step in range(ITERS):
        if step == 0:
            for load in loads:
                load.wait()
            facg[...] = jnp.exp(-time_step * (ext_v[...] + den_v[...] - energy_shift))

            def forward(n, carry):
                w = []
                for c in range(2 * PF):
                    at = n * 2 * PF + c
                    f = facg[at % 8]
                    w.append(jnp.concatenate(
                        [bands_v[p, at // 8, at % 8].astype(F32) * f for p in range(2)], axis=1
                    ).astype(BF16))
                for c, b in enumerate(forward_zy(jnp.concatenate(w, axis=0))):
                    send_f[pl.ds((n * 2 * PF + c) * 8, 8)] = b
                return carry

            lax.fori_loop(0, 8 // PF, forward, 0)
            pl.semaphore_wait(barrier, 150)

            def first_sends(n, carry):
                which, j = n // 8, n % 8
                for k, q in enumerate(columns):
                    send_tile(
                        send_f.at[n * 8 + q], recv_f.at[8 * i + j], sf_sem, rf_sem, g, 2 * q + which,
                        which == core if k == 7 else None,
                    )
                return carry

            lax.fori_loop(0, 16, first_sends, 0)
            for copy in late:
                copy.start()


            @pl.when(owner)
            def _():
                pieces = [
                    (ext.at[zz], plane.at[0], 0), (den.at[zz], plane.at[1], 0),
                    (pden.at[zz], plane.at[2], 0), (pres.at[zz], plane.at[3], 0),
                    (hden.at[:, zz], rs.at[pl.ds(0, DEPTH - 1)], 1),
                    (hres.at[:, zz], qs.at[pl.ds(0, DEPTH - 1)], 2),
                ]
                for src, dst, s in pieces:
                    pltpu.make_async_copy(src, dst, pl_sems.at[s]).start()
                    remote(src, dst, pl_send.at[s], pl_sems.at[s], g, twin).start()

            occ_row = jnp.full((1, NG), occ[core], F32)
            occ_s[...] = occ_row
            occs[g] = occ_row

            def send_occ(n, c):
                remote(occ_s, occs.at[g], so_sem, ro_sem, (g + n) % 16, i).start()
                return c

            lax.fori_loop(1, 16, send_occ, 0)

        else:
            def forward(n, carry):
                ts = bands_of(n, PF)
                f = facp[...]
                f = jnp.concatenate([f, f], axis=1)
                w = jnp.concatenate([(psi[t].astype(F32) * f).astype(BF16) for t in ts], axis=0)
                for t, b in zip(ts, forward_zy(w)):
                    send_f[pl.ds(t * 8, 8)] = b
                return carry

            lax.fori_loop(0, 8 // PF, forward, 0)
            pltpu.make_async_copy(send_f.at[g * 8 + xy], recv_f.at[me], rf_sem).start()
            for n, at in far_first:
                q, dg = columns[n], rings[at]
                send_tile(
                    send_f.at[dg * 8 + q], recv_f.at[me], sf_sem, rf_sem, dg, 2 * q + core
                )

        if step:
            if step == 1:
                for copy in late:
                    copy.wait()
            slab_update(step - 1)
        spectral()
        drain(send_f.at[pl.ds(0, 120 if step == 0 else 127)], sf_sem)

        if step == 0:
            drain(plane, pl_sems.at[0])
            drain(rs.at[pl.ds(0, DEPTH - 1)], pl_sems.at[1])
            drain(qs.at[pl.ds(0, DEPTH - 1)], pl_sems.at[2])
            drain(occs.at[pl.ds(0, 15)], ro_sem)
            drain(occs.at[pl.ds(0, 15)], so_sem)

            @pl.when(owner)
            def _():
                drain(plane, pl_send.at[0])
                drain(rs.at[pl.ds(0, DEPTH - 1)], pl_send.at[1])
                drain(qs.at[pl.ds(0, DEPTH - 1)], pl_send.at[2])

        lanes = lax.broadcasted_iota(jnp.int32, (1, NG), 1)
        row = jnp.zeros((1, NG), F32)

        def put(row, at, a, b):
            total = jnp.sum(jnp.sum(rows_of(a * b), axis=0), axis=0, keepdims=True)
            return jnp.where(lanes == at, jnp.sum(total, axis=1, keepdims=True), row)

        if step == 0:
            at = 2 * DEPTH
            for a in range(DEPTH - 1):
                for b in range(a + 1):
                    row = put(row, at, qs[a], qs[b])
                    at += 1

        part[...] = jnp.zeros_like(part)
        lax.fori_loop(0, 8 // PB, functools.partial(backward, keep=step < ITERS - 1), 0)

        swap = remote(part, recv_d.at[step], sd_sem, rd_sems.at[step], g, twin)
        swap.start()
        swap.wait_recv()
        rho_out = (part[...] + recv_d[step]) * (density_scale / bands_total)
        rho_in = plane[1]
        res = rho_out - rho_in
        newest = res - plane[3]
        rs[DEPTH - 1 + step] = rho_in - plane[2]
        qs[DEPTH - 1 + step] = newest

        for j in range(DEPTH):
            q = qs[step + j]
            row = put(row, j, q, newest)
            row = put(row, DEPTH + j, q, res)
        row_s[...] = row
        rows[me] = row

        for n, at in far_first:
            remote(
                row_s, rows.at[me], sr_sem, rr_sem, rings[at], 2 * columns[n] + core
            ).start()

        outs_s[step] = res.astype(BF16)

        def send_res(m, carry):
            z = z_of(m)
            for h in range(2):
                send_tile(
                    outs_s.at[step, pl.ds(pl.multiple_of(core * KEPT, KEPT), KEPT)],
                    res_v.at[step, 2 * zz + core], sout_sems.at[step], rout_sems.at[step],
                    halves[h] * 8 + z, 2 * xy + half,
                    jnp.logical_and(m == 7, owner) if h == 1 else None,
                )
            return carry

        lax.fori_loop(0, 8, send_res, 0)

        if step == ITERS - 1:
            def join(j, carry):
                for k in range(step, step + DEPTH - 1):
                    rslab[k, j] = rslab[k, j] + mixing_weight * qslab[k, j]
                return carry

            lax.fori_loop(0, 8, join, 0)

        swap.wait_send()
        drain(rows.at[pl.ds(0, 127)], rr_sem)
        drain(rows.at[pl.ds(0, 127)], sr_sem)
        drain(send_b.at[pl.ds(0, 127)], sb_sem)
        sums = jnp.sum(rows[...], axis=0) * (1.0 / (NG * NG * NG))

        def splat(at):
            return jnp.broadcast_to(sums[:, at : at + 1], (8, NG))

        border = [splat(j) for j in range(DEPTH)]
        right = [splat(DEPTH + j) for j in range(DEPTH)]
        if step == 0:
            at = 2 * DEPTH
            gram = []
            for a in range(DEPTH - 1):
                gram.append([splat(at + b) for b in range(a + 1)])
                at += a + 1
        else:
            gram = [[gram[a][b] for b in range(1, a + 1)] for a in range(1, DEPTH)]
        gram.append(border)
        trace = gram[0][0]
        for j in range(1, DEPTH):
            trace = trace + gram[j][j]
        ridge = trace * (ridge_share / DEPTH) + ridge_floor
        low = [[None] * DEPTH for _ in range(DEPTH)]
        scaled = [[None] * DEPTH for _ in range(DEPTH)]
        inverse = [None] * DEPTH
        for c in range(DEPTH):
            value = gram[c][c] + ridge
            for k in range(c):
                value = value - scaled[c][k] * low[c][k]
            inverse[c] = 1.0 / value
            for r in range(c + 1, DEPTH):
                value = gram[r][c]
                for k in range(c):
                    value = value - scaled[r][k] * low[c][k]
                scaled[r][c] = value
                low[r][c] = value * inverse[c]
        middle = []
        for r in range(DEPTH):
            value = right[r]
            for k in range(r):
                value = value - low[r][k] * middle[k]
            middle.append(value)
        coeffs = [None] * DEPTH
        for r in reversed(range(DEPTH)):
            value = middle[r] * inverse[r]
            for k in range(r + 1, DEPTH):
                value = value - low[k][r] * coeffs[k]
            coeffs[r] = value
        for k in range(DEPTH):
            coef_v[step, k] = coeffs[k]
        if step == ITERS - 1:
            break
        mixed = rows_of(rho_in + mixing_weight * res)
        for j in range(DEPTH):
            mixed = mixed - coeffs[j][None] * rows_of(rs[step + j] + mixing_weight * qs[step + j])
        rho = mixed.reshape(NG, NG)
        plane[2] = rho_in
        plane[3] = res
        plane[1] = rho
        facp[...] = jnp.exp(-time_step * (plane[0] + rho - energy_shift))

    slab_update(ITERS - 1)
    for step in range(ITERS):
        @pl.when(owner)
        def _():
            drain(res_v.at[step, pl.ds(0, 15)], sout_sems.at[step])

        @pl.when(jnp.logical_not(owner))
        def _():
            drain(res_v.at[step], sout_sems.at[step])


def local(bands, occupations, external, density_in, prev_density, prev_residual, hist_density, hist_residual):
    slab = external.shape
    hbm = pl.BlockSpec(memory_space=pltpu.HBM)
    smem = pl.BlockSpec(memory_space=pltpu.SMEM)
    dma = pltpu.SemaphoreType.DMA
    both = pl.pallas_call(
        kernel,
        out_shape=[jax.ShapeDtypeStruct((16, KEPT, NG), BF16)] * 2,
        in_specs=[smem] + [hbm] * 8,
        out_specs=[hbm] * 2,
        scratch_shapes=[
            pltpu.VMEM((6 * NG, NG), BF16),
            pltpu.VMEM(bands.shape, BF16),
            pltpu.VMEM(slab, F32),
            pltpu.VMEM(slab, F32),
            pltpu.VMEM(slab, F32),
            pltpu.VMEM((NG, NG), F32),
            pltpu.VMEM((4, NG, NG), F32),
            pltpu.VMEM((DEPTH - 1 + ITERS, NG, NG), F32),
            pltpu.VMEM((DEPTH - 1 + ITERS, NG, NG), F32),
            pltpu.VMEM((16, NG, 2 * NG), BF16),
            pltpu.VMEM((128, 8, NG), BF16),
            pltpu.VMEM((128, 8, NG), BF16),
            pltpu.VMEM((8 * NG, NG), F32),
            pltpu.VMEM((8, KEPT, NG), F32),
            pltpu.VMEM((128, 8, NG), BF16),
            pltpu.VMEM((128, 8, NG), BF16),
            pltpu.VMEM((NG, NG), F32),
            pltpu.VMEM((ITERS, NG, NG), F32),
            pltpu.VMEM((1, NG), F32),
            pltpu.VMEM((128, 1, NG), F32),
            pltpu.VMEM((1, NG), F32),
            pltpu.VMEM((16, 1, NG), F32),
            pltpu.VMEM((ITERS, NG, NG), BF16),
            pltpu.VMEM((ITERS, 16, KEPT, NG), BF16),
            pltpu.VMEM((16, KEPT, NG), BF16),
            pltpu.VMEM((DEPTH - 1 + ITERS, *slab), F32),
            pltpu.VMEM((DEPTH - 1 + ITERS, *slab), F32),
            pltpu.VMEM(slab, F32),
            pltpu.VMEM(slab, F32),
            pltpu.VMEM((ITERS, DEPTH, 8, NG), F32),
            dma((4,)), dma((3,)), dma((3,)),
            dma(()), dma(()), dma(()), dma((16,)), dma(()), dma((ITERS,)),
            dma(()), dma(()), dma(()), dma(()), dma((ITERS,)), dma((ITERS,)), dma((4,)), dma((2,)),
        ],
        compiler_params=pltpu.CompilerParams(
            has_side_effects=True, collective_id=0, vmem_limit_bytes=67043328
        ),
        name="scf",
    )(
        occupations, bands, external, density_in, prev_density, prev_residual,
        hist_density, hist_residual, jnp.asarray(tables()),
    )
    return tuple(half.reshape(slab).astype(F32) for half in both)


def solution(mesh):
    placed = (
        P(None, "band", "grid", None, None),
        P("band"),
        P("grid", None, None),
        P("grid", None, None),
        P("grid", None, None),
        P("grid", None, None),
        P(None, "grid", None, None),
        P(None, "grid", None, None),
    )
    return jax.shard_map(
        local,
        mesh=mesh,
        in_specs=placed,
        out_specs=(P("grid", None, None), P("grid", None, None)),
        check_vma=False,
    )
```
